8 devices in a mesh: rep: 1 (over z), dp: 8 (over x, y, core).
Axes of the slice: x: 2, y: 2, z: 1, core: 2. Of those that a mesh axis runs over, the one named last changes fastest.
Arguments:
- x: bfloat16 [8, 2048, 1024], P(('rep', 'dp'))
- dy: bfloat16 [8, 2048, 1024], P(('rep', 'dp'))
- wq: bfloat16 [2, 1024, 1024], replicated
- wk: bfloat16 [2, 1024, 1024], replicated
- wv: bfloat16 [2, 1024, 1024], replicated
- wo: bfloat16 [2, 1024, 1024], replicated
- w_gate: bfloat16 [2, 1024, 4096], replicated
- w_up: bfloat16 [2, 1024, 4096], replicated
- w_down: bfloat16 [2, 4096, 1024], replicated
- m_wq: float32 [2, 1024, 1024], P(None, 'dp')
- m_wk: float32 [2, 1024, 1024], P(None, 'dp')
- m_wv: float32 [2, 1024, 1024], P(None, 'dp')
- m_wo: float32 [2, 1024, 1024], P(None, 'dp')
- m_w_gate: float32 [2, 1024, 4096], P(None, 'dp')
- m_w_up: float32 [2, 1024, 4096], P(None, 'dp')
- m_w_down: float32 [2, 4096, 1024], P(None, 'dp')
- v_wq: float32 [2, 1024, 1024], P(None, 'dp')
- v_wk: float32 [2, 1024, 1024], P(None, 'dp')
- v_wv: float32 [2, 1024, 1024], P(None, 'dp')
- v_wo: float32 [2, 1024, 1024], P(None, 'dp')
- v_w_gate: float32 [2, 1024, 4096], P(None, 'dp')
- v_w_up: float32 [2, 1024, 4096], P(None, 'dp')
- v_w_down: float32 [2, 4096, 1024], P(None, 'dp')
Outputs:
- output 1: bfloat16 [2, 1024, 1024], P('rep')
- output 2: bfloat16 [2, 1024, 1024], P('rep')
- output 3: bfloat16 [2, 1024, 1024], P('rep')
- output 4: bfloat16 [2, 1024, 1024], P('rep')
- output 5: bfloat16 [2, 1024, 4096], P('rep')
- output 6: bfloat16 [2, 1024, 4096], P('rep')
- output 7: bfloat16 [2, 4096, 1024], P('rep')
- output 8: float32 [2, 1024, 1024], P('rep', 'dp')
- output 9: float32 [2, 1024, 1024], P('rep', 'dp')
- output 10: float32 [2, 1024, 1024], P('rep', 'dp')
- output 11: float32 [2, 1024, 1024], P('rep', 'dp')
- output 12: float32 [2, 1024, 4096], P('rep', 'dp')
- output 13: float32 [2, 1024, 4096], P('rep', 'dp')
- output 14: float32 [2, 4096, 1024], P('rep', 'dp')
- output 15: float32 [2, 1024, 1024], P('rep', 'dp')
- output 16: float32 [2, 1024, 1024], P('rep', 'dp')
- output 17: float32 [2, 1024, 1024], P('rep', 'dp')
- output 18: float32 [2, 1024, 1024], P('rep', 'dp')
- output 19: float32 [2, 1024, 4096], P('rep', 'dp')
- output 20: float32 [2, 1024, 4096], P('rep', 'dp')
- output 21: float32 [2, 4096, 1024], P('rep', 'dp')
All inputs are finite; a program needn't handle non-finite values.
Results may differ from the reference program's by a relative error of at most 0.024.
Values are sent between devices in bfloat16 or wider.
A program may use at most 2 GiB of HBM per device.

```python
import jax
import jax.numpy as jnp
from jax import lax

SEQUENCES = 8
TOKENS = 2048
D = 1024
HEADS = 4
KV_HEADS = 4
HEAD = 256
FF = 4096
LAYERS = 2
THETA = 10000
NAMES = ("wq", "wk", "wv", "wo", "w_gate", "w_up", "w_down")
SHAPES = {
    "wq": (LAYERS, D, HEADS * HEAD),
    "wk": (LAYERS, D, KV_HEADS * HEAD),
    "wv": (LAYERS, D, KV_HEADS * HEAD),
    "wo": (LAYERS, HEADS * HEAD, D),
    "w_gate": (LAYERS, D, FF),
    "w_up": (LAYERS, D, FF),
    "w_down": (LAYERS, FF, D),
}


def bump(key, n, height):
    away = (jnp.arange(n, dtype=jnp.int32) - jax.random.randint(key, (), 0, n, jnp.int32)) % n
    return jnp.where(away < n // 8, height, 1.0)


def together(key, own, strength):
    shared = jax.random.normal(key, own.shape[1:], jnp.float32)
    return (own + strength * shared) * lax.rsqrt(1 + strength * strength)


def setup_inputs(seed: int = 0, part: int = 0) -> dict:
    kx, kdy, ka, kb, kz, kf, kh, kl, *keys = jax.random.split(jax.random.key(seed), 8 + 3 * len(NAMES))
    kx, kdy, ka, kb = (jax.random.fold_in(k, part) for k in (kx, kdy, ka, kb))
    kw, km, kv = (keys[i::3] for i in range(3))
    shape = (SEQUENCES, TOKENS, D)
    much_x, much_dy = jax.random.uniform(kz, (2,), jnp.float32, 0.0, 1.0)
    loud = 2.0 ** jax.random.uniform(jax.random.fold_in(kz, 1), (), jnp.float32, -1.0, 2.0)
    layers = 2.0 ** jax.random.uniform(kl, (LAYERS, 1, 1), jnp.float32, -1.0, 1.0)
    times = {"wq": 1.0, "wk": 1.0, "wv": 2.0, "wo": layers, "w_gate": 1.0, "w_up": bump(kh, FF, 4.0), "w_down": layers}
    x = together(ka, jax.random.normal(kx, shape, jnp.float32), much_x) * bump(kf, D, 4.0)
    dy = together(kb, jax.random.normal(kdy, shape, jnp.float32), much_dy)
    drawn = {"x": x.astype(jnp.bfloat16), "dy": (loud * dy * (SEQUENCES * TOKENS) ** -0.5).astype(jnp.bfloat16)}
    for key, name in zip(kw, NAMES, strict=True):
        drawn[name] = (jax.random.normal(key, SHAPES[name], jnp.float32) * SHAPES[name][1] ** -0.5 * times[name]).astype(jnp.bfloat16)
    for key, name in zip(km, NAMES, strict=True):
        drawn[f"m_{name}"] = 0.1 * jax.random.normal(key, SHAPES[name], jnp.float32)
    for key, name in zip(kv, NAMES, strict=True):
        drawn[f"v_{name}"] = jax.random.uniform(key, SHAPES[name], jnp.float32, 0.02, 0.06)
    return drawn


def matmul(a, w):
    return jnp.dot(a, w, preferred_element_type=jnp.float32).astype(jnp.bfloat16)


def normed(h):
    wide = h.astype(jnp.float32)
    scale = lax.rsqrt(jnp.mean(wide**2, -1, keepdims=True) + 1e-6)
    return (wide * scale).astype(jnp.bfloat16)


def turned(t, theta):
    half = t.shape[-1] // 2
    angle = jnp.arange(t.shape[0], dtype=jnp.float32)[:, None] * theta ** (-jnp.arange(half, dtype=jnp.float32) / half)
    cos, sin = jnp.cos(angle)[:, None], jnp.sin(angle)[:, None]
    a, b = t[..., :half].astype(jnp.float32), t[..., half:].astype(jnp.float32)
    return jnp.concatenate([a * cos - b * sin, b * cos + a * sin], -1).astype(jnp.bfloat16)


def seen_by(q, k, v):
    tokens, kv = q.shape[0], k.shape[1]
    q = q.reshape(tokens, kv, -1, q.shape[-1])
    scores = jnp.einsum("tgsd,ugd->gstu", q.astype(jnp.float32), k.astype(jnp.float32)) * q.shape[-1] ** -0.5
    place = jnp.arange(tokens)
    weights = jax.nn.softmax(jnp.where(place[:, None] >= place, scores, -jnp.inf), -1).astype(jnp.bfloat16)
    return jnp.einsum("gstu,ugd->tgsd", weights.astype(jnp.float32), v.astype(jnp.float32)).astype(jnp.bfloat16).reshape(tokens, -1)


def layer(h, w):
    a = normed(h)
    q, k = (turned(matmul(a, w[name]).reshape(h.shape[0], -1, HEAD), THETA) for name in ("wq", "wk"))
    h = h + matmul(seen_by(q, k, matmul(a, w["wv"]).reshape(h.shape[0], -1, HEAD)), w["wo"])
    b = normed(h)
    gate = jnp.dot(b, w["w_gate"], preferred_element_type=jnp.float32)
    up = jnp.dot(b, w["w_up"], preferred_element_type=jnp.float32)
    return h + matmul((jax.nn.silu(gate) * up).astype(jnp.bfloat16), w["w_down"])


def adamw(w, m, v, g):
    m = 0.9 * m + 0.1 * g
    v = 0.95 * v + 0.05 * g * g
    step = m * lax.rsqrt(v + 1e-8) + 0.1 * w
    return (w - 0.02 * step).astype(jnp.bfloat16), m, v


def clipped(gradients, sum_of_squares, count):
    factor = jnp.minimum(1.0, 0.5 * lax.rsqrt(sum_of_squares / count + 1e-30))
    return [g * factor for g in gradients]


def stack(weights, h):
    return lax.scan(lambda h, w: (layer(h, w), None), h, weights)[0]


def reference(x, dy, wq, wk, wv, wo, w_gate, w_up, w_down, m_wq, m_wk, m_wv, m_wo, m_w_gate, m_w_up, m_w_down, v_wq, v_wk, v_wv, v_wo, v_w_gate, v_w_up, v_w_down):
    weights = dict(zip(NAMES, (wq, wk, wv, wo, w_gate, w_up, w_down), strict=True))

    def take(so_far, sequence):
        h, by_y = sequence
        _, back = jax.vjp(stack, weights, h)
        by_weights, by_h = back(by_y)
        return jax.tree.map(lambda total, term: total + term.astype(jnp.float32), so_far, by_weights), by_h

    none_yet = {name: jnp.zeros(w.shape, jnp.float32) for name, w in weights.items()}
    by_weights, by_x = lax.scan(take, none_yet, (x, dy))
    gradients = [by_weights[name].astype(jnp.bfloat16).astype(jnp.float32) for name in NAMES]
    gradients = clipped(gradients, sum(jnp.sum(g * g) for g in gradients), sum(g.size for g in gradients))
    first = (m_wq, m_wk, m_wv, m_wo, m_w_gate, m_w_up, m_w_down)
    second = (v_wq, v_wk, v_wv, v_wo, v_w_gate, v_w_up, v_w_down)
    new = [adamw(weights[name].astype(jnp.float32), m, v, g) for name, m, v, g in zip(NAMES, first, second, gradients, strict=True)]
    return tuple(one[which] for which in range(3) for one in new)
```

```python
import functools

import jax
import jax.numpy as jnp
from jax import lax
from jax.experimental import pallas as pl
from jax.experimental.pallas import tpu as pltpu
from jax.sharding import PartitionSpec as P

NEG = -1e30
HIDDEN = 2 * NEG
LOG2E = 1.4426950408889634
VMEM = 63 * 2**20
HEAD = 256
HALF = HEAD // 2
THETA = 10000
NAMES = ("wq", "wk", "wv", "wo", "w_gate", "w_up", "w_down")
F32, BF16 = jnp.float32, jnp.bfloat16


def _dot(a, b, ca=1, cb=0):
    return lax.dot_general(a, b, (((ca,), (cb,)), ((), ())), preferred_element_type=F32)


def _call(kernel, name, grid, ins, outs, scratch, flops, args):
    def spec(block, index, still=False):
        return pl.BlockSpec(block, index, pipeline_mode=pl.Buffered(1)) if still else pl.BlockSpec(block, index)

    shapes = [jax.ShapeDtypeStruct(o[2], o[3]) for o in outs]
    moved = sum(a.size * a.dtype.itemsize for a in (*args, *shapes))
    return pl.pallas_call(
        kernel,
        name=name,
        grid=grid,
        in_specs=[spec(*i) for i in ins],
        out_specs=[spec(o[0], o[1]) for o in outs],
        out_shape=shapes,
        scratch_shapes=scratch,
        compiler_params=pltpu.CompilerParams(dimension_semantics=("arbitrary",) * len(grid), vmem_limit_bytes=VMEM),
        cost_estimate=pl.CostEstimate(flops=flops, transcendentals=0, bytes_accessed=moved),
    )(*args)


def _mask(bk, wide, shift):
    return lax.broadcasted_iota(jnp.int32, (bk, wide), 1) + shift >= lax.broadcasted_iota(jnp.int32, (bk, wide), 0)


def _cols(i):
    return slice(i * HEAD, (i + 1) * HEAD)


def _attend(q_ref, k_ref, v_ref, o_ref, lse_ref, top_s, mix_s, *, scale, bq, bk, heads):
    iq = pl.program_id(1)
    e = scale * LOG2E
    wide = bk
    top_s[...] = jnp.full(top_s.shape, NEG, F32)
    mix_s[...] = jnp.zeros(mix_s.shape, F32)
    ones = jnp.ones((8, bk), BF16)

    def block(j, strips):
        here = pl.ds(pl.multiple_of(j * bk, bk), bk)
        pieces = [(i, at, cut) for i in range(heads) for at, cut in strips]
        scores = [_dot(k_ref[here, _cols(i)], q_ref[at : at + wide, _cols(i)], 1, 1) for i, at, _ in pieces]
        weights, keeps = [], []
        for (i, at, cut), s in zip(pieces, scores):
            if cut:
                s = jnp.where(_mask(bk, wide, 0), s, HIDDEN)
            old = top_s[i : i + 1, at : at + wide]
            top = jnp.maximum(old, s.max(axis=0, keepdims=True))
            top_s[i : i + 1, at : at + wide] = top
            weights.append(jnp.exp2((s - top) * e).astype(BF16))
            keeps.append(jnp.exp2((old - top) * e))
        for (i, at, _), p, keep in zip(pieces, weights, keeps):
            values = jnp.concatenate([v_ref[here, _cols(i)].T, ones], axis=0)
            mix_s[i, :, at : at + wide] = mix_s[i, :, at : at + wide] * keep + _dot(values, p)

    n = bq // bk
    lax.fori_loop(0, iq * n, lambda j, _: block(j, [(at, False) for at in range(0, bq, wide)]), None)
    for d in range(n):
        block(iq * n + d, [(at, at == d * bk) for at in range(d * bk, bq, wide)])
    for i in range(heads):
        top, total = top_s[i : i + 1, :], mix_s[i, HEAD : HEAD + 1, :]
        o_ref[:, _cols(i)] = (mix_s[i, :HEAD, :] * (1 / total)).T.astype(BF16)
        lse_ref[i : i + 1, :] = top * scale + jnp.log(total)


def attend(q, k, v):
    t, width = q.shape
    heads, bq, bk = width // HEAD, min(1024, t), min(512, t)
    return _call(
        functools.partial(_attend, scale=HEAD**-0.5, bq=bq, bk=bk, heads=heads),
        "attend",
        (1, t // bq),
        [((bq, width), lambda ih, iq: (iq, 0)), ((t, width), lambda ih, iq: (0, 0), True), ((t, width), lambda ih, iq: (0, 0), True)],
        [((bq, width), lambda ih, iq: (iq, 0), (t, width), BF16), ((heads, bq), lambda ih, iq: (0, iq), (heads, t), F32)],
        [pltpu.VMEM((heads, bq), F32), pltpu.VMEM((heads, HEAD + 8, bq), F32)],
        2 * t * t * width,
        (q, k, v),
    )


def _turn(x, cos, sin, back=False):
    a, b = x[:, :HALF], x[:, HALF:]
    if back:
        return jnp.concatenate([a * cos + b * sin, b * cos - a * sin], axis=1)
    return jnp.concatenate([a * cos - b * sin, b * cos + a * sin], axis=1)


def _attend_back(q_ref, k_ref, v_ref, do_ref, o_ref, lse_ref, cosq_ref, sinq_ref, cos_ref, sin_ref, dq_ref, dk_ref, dv_ref, dq_s, dk_s, dv_s,
                 delta_s, lse_s, *, scale, bq, bk, heads):
    ih, iq = pl.program_id(0), pl.program_id(1)
    e = scale * LOG2E
    wide = bk

    @pl.when(iq == 0)
    def _():
        dk_s[...] = jnp.zeros_like(dk_s)
        dv_s[...] = jnp.zeros_like(dv_s)

    dq_s[...] = jnp.zeros_like(dq_s)
    for i in range(heads):
        delta_s[i : i + 1, :] = (do_ref[:, _cols(i)].astype(F32) * o_ref[:, _cols(i)].astype(F32)).T.sum(axis=0, keepdims=True)
        lse_s[i : i + 1, :] = lse_ref[0, i : i + 1, :] * LOG2E

    def block(j, strips):
        here = pl.ds(pl.multiple_of(j * bk, bk), bk)
        pieces = [(i, at, cut) for i in range(heads) for at, cut in strips]
        qs = [q_ref[at : at + wide, _cols(i)] for i, at, _ in pieces]
        dos = [do_ref[at : at + wide, _cols(i)] for i, at, _ in pieces]
        scores = [_dot(k_ref[here, _cols(i)], x, 1, 1) for (i, _, _), x in zip(pieces, qs)]
        dps = [_dot(v_ref[here, _cols(i)], x, 1, 1) for (i, _, _), x in zip(pieces, dos)]
        for n, (i, at, cut) in enumerate(pieces):
            p = jnp.exp2(scores[n] * e - lse_s[i : i + 1, at : at + wide])
            if cut:
                p = jnp.where(_mask(bk, wide, 0), p, 0.0)
            ds = (p * (dps[n] - delta_s[i : i + 1, at : at + wide])).astype(BF16)
            dv_s[i, here, :] += _dot(p.astype(BF16), dos[n])
            dk_s[i, here, :] += _dot(ds, qs[n])
            dq_s[i, :, at : at + wide] += _dot(k_ref[here, _cols(i)].T, ds)

    n = bq // bk
    lax.fori_loop(0, iq * n, lambda j, _: block(j, [(at, False) for at in range(0, bq, wide)]), None)
    for d in range(n):
        block(iq * n + d, [(at, at == d * bk) for at in range(d * bk, bq, wide)])
    for i in range(heads):
        dq_ref[:, _cols(i)] = _turn((dq_s[i] * scale).T.astype(BF16).astype(F32), cosq_ref[...], sinq_ref[...], True).astype(BF16)

    @pl.when(iq == pl.num_programs(1) - 1)
    def _():
        for i in range(heads):
            dk_ref[:, _cols(i)] = _turn((dk_s[i] * scale).astype(BF16).astype(F32), cos_ref[...], sin_ref[...], True).astype(BF16)
            dv_ref[:, _cols(i)] = dv_s[i].astype(BF16)


def attend_back(q, k, v, d_out, out, lse, cos, sin):
    t, width = q.shape
    heads, bq, bk = 2, min(1024, t), min(512, t)
    cols = heads * HEAD
    queries = ((bq, cols), lambda ih, iq: (iq, ih))
    keys = ((t, cols), lambda ih, iq: (0, ih))
    stats = ((1, heads, bq), lambda ih, iq: (ih, 0, iq))
    table_q = ((bq, HALF), lambda ih, iq: (iq, 0))
    table = ((t, HALF), lambda ih, iq: (0, 0), True)
    return _call(
        functools.partial(_attend_back, scale=HEAD**-0.5, bq=bq, bk=bk, heads=heads),
        "attend_back",
        (width // cols, t // bq),
        [queries, keys, keys, queries, queries, stats, table_q, table_q, table, table],
        [(*queries, (t, width), BF16), (*keys, (t, width), BF16), (*keys, (t, width), BF16)],
        [pltpu.VMEM((heads, HEAD, bq), F32), pltpu.VMEM((heads, t, HEAD), F32), pltpu.VMEM((heads, t, HEAD), F32),
         pltpu.VMEM((heads, bq), F32), pltpu.VMEM((heads, bq), F32)],
        5 * t * t * width,
        (q, k, v, d_out, out, lse.reshape(-1, heads, t), cos, sin, cos, sin),
    )


ROWS = 512
TILE = 512


def _scale_of(h):
    return lax.rsqrt(jnp.mean(h * h, axis=-1, keepdims=True) + 1e-6)


def _norm(h):
    return (h * _scale_of(h)).astype(BF16)


def _norm_back(by, h):
    r = _scale_of(h)
    return (by * r - h * (r * r * r * jnp.mean(by * h, axis=-1, keepdims=True))).astype(BF16)


def _qkv(h_ref, wq_ref, wk_ref, wv_ref, cos_ref, sin_ref, a_ref, q_ref, k_ref, v_ref):
    a = _norm(h_ref[...].astype(F32))
    a_ref[...] = a
    cos, sin = cos_ref[...], sin_ref[...]
    for i in range(q_ref.shape[1] // HEAD):
        for w_ref, to_ref in ((wq_ref, q_ref), (wk_ref, k_ref)):
            t = _dot(a, w_ref[0, :, _cols(i)]).astype(BF16).astype(F32)
            to_ref[:, _cols(i)] = _turn(t, cos, sin).astype(BF16)
        v_ref[:, _cols(i)] = _dot(a, wv_ref[0, :, _cols(i)]).astype(BF16)


def qkv(h, wq, wk, wv, cos, sin, number):
    t, d = h.shape
    width = wq.shape[2]
    rows = ((ROWS, d), lambda i: (i, 0))
    wide = ((ROWS, width), lambda i: (i, 0))
    w = ((1, d, width), lambda i: (number, 0, 0), True)
    table = ((ROWS, HALF), lambda i: (i, 0))
    return _call(_qkv, "qkv", (t // ROWS,), [rows, w, w, w, table, table],
                 [(*rows, (t, d), BF16)] + [(*wide, (t, width), BF16)] * 3, [], 6 * t * d * width, (h, wq, wk, wv, cos, sin))


def _out(h_ref, o_ref, w_ref, h2_ref, b_ref):
    h2 = (h_ref[...].astype(F32) + _dot(o_ref[...], w_ref[0]).astype(BF16).astype(F32)).astype(BF16)
    h2_ref[...] = h2
    b_ref[...] = _norm(h2.astype(F32))


def out_and_norm(h, o, wo, number):
    t, d = h.shape
    width = o.shape[1]
    rows, wide = ((ROWS, d), lambda i: (i, 0)), ((ROWS, width), lambda i: (i, 0))
    return _call(_out, "out", (t // ROWS,), [rows, wide, ((1, width, d), lambda i: (number, 0, 0), True)],
                 [(*rows, (t, d), BF16)] * 2, [], 2 * t * d * width, (h, o, wo))


def _mlp(b_ref, h_ref, wg_ref, wu_ref, wd_ref, g_ref, u_ref, to_ref, sum_s):
    f = pl.program_id(0)
    for at in range(0, b_ref.shape[0], ROWS):
        here = slice(at, at + ROWS)
        b = b_ref[here, :]
        g, u = _dot(b, wg_ref[0]), _dot(b, wu_ref[0])
        g_ref[here, :], u_ref[here, :] = g, u
        term = _dot((g * jax.nn.sigmoid(g) * u).astype(BF16), wd_ref[0])
        sum_s[here, :] = jnp.where(f == 0, term, sum_s[here, :] + term)

    @pl.when(f == pl.num_programs(0) - 1)
    def _():
        to_ref[...] = (h_ref[...].astype(F32) + sum_s[...].astype(BF16).astype(F32)).astype(BF16)


def _tiles(d, number):
    up = ((1, d, TILE), lambda i: (number, 0, i))
    down = ((1, TILE, d), lambda i: (number, i, 0))
    return up, down


def mlp(b, h, wg, wu, wd, number):
    t, d = b.shape
    ff = wg.shape[2]
    up, down = _tiles(d, number)
    whole = ((t, d), lambda i: (0, 0), True)
    hidden = ((t, TILE), lambda i: (0, i))
    return _call(_mlp, "mlp", (ff // TILE,), [whole, whole, up, up, down],
                 [(*hidden, (t, ff), F32)] * 2 + [((t, d), lambda i: (0, 0), (t, d), BF16)], [pltpu.VMEM((t, d), F32)], 6 * t * d * ff,
                 (b, h, wg, wu, wd))


def _mlp_back(dh_ref, wd_ref, g_of, u_of, dg_ref, du_ref, dwd_ref, act_s):
    for at in range(0, dh_ref.shape[0], ROWS):
        here = slice(at, at + ROWS)
        g, u = g_of(here), u_of(here)
        by = _dot(dh_ref[here, :], wd_ref[0], 1, 1).astype(BF16).astype(F32)
        s = jax.nn.sigmoid(g)
        silu = g * s
        act_s[here, :] = (silu * u).astype(BF16)
        du_ref[here, :] = (by * silu).astype(BF16)
        dg_ref[here, :] = (by * u * (s + silu * (1 - s))).astype(BF16)
    dwd_ref[...] = _dot(act_s[...].T, dh_ref[...]).astype(BF16)


def _mlp_back_anew(b_ref, dh_ref, wg_ref, wu_ref, wd_ref, *rest):
    _mlp_back(dh_ref, wd_ref, lambda here: _dot(b_ref[here, :], wg_ref[0]), lambda here: _dot(b_ref[here, :], wu_ref[0]), *rest)


def _mlp_back_kept(g_ref, u_ref, dh_ref, wd_ref, *rest):
    _mlp_back(dh_ref, wd_ref, lambda here: g_ref[here, :], lambda here: u_ref[here, :], *rest)


def mlp_back(kept, dh, wg, wu, wd, number):
    t, d = dh.shape
    ff = wg.shape[2]
    up, down = _tiles(d, number)
    whole = ((t, d), lambda i: (0, 0), True)
    hidden = ((t, TILE), lambda i: (0, i))
    if len(kept) == 2:
        kernel, ins, args, work = _mlp_back_kept, [hidden, hidden, whole, down], (*kept, dh, wd), 4
    else:
        kernel, ins, args, work = _mlp_back_anew, [whole, whole, up, up, down], (*kept, dh, wg, wu, wd), 8
    return _call(kernel, "mlp_back", (ff // TILE,), ins,
                 [(*hidden, (t, ff), BF16)] * 2 + [((TILE, d), lambda i: (i, 0), (ff, d), BF16)], [pltpu.VMEM((t, TILE), BF16)],
                 work * t * d * ff, args)


def _up_back(dg_ref, du_ref, b_ref, h_ref, dh_ref, wg_ref, wu_ref, wo_ref, dw_ref, dh2_ref, do_ref, bt_s, sum_s):
    f = pl.program_id(0)
    n, d = dw_ref.shape[0], b_ref.shape[1]

    @pl.when(f == 0)
    def _():
        bt_s[...] = b_ref[...].T

    for i, ref in enumerate((dg_ref, du_ref)):
        dw_ref[:, i] = _dot(bt_s[...], ref[...]).astype(BF16).reshape(n, d // n, TILE)
    for at in range(0, b_ref.shape[0], ROWS):
        here = slice(at, at + ROWS)
        term = _dot(dg_ref[here, :], wg_ref[0], 1, 1) + _dot(du_ref[here, :], wu_ref[0], 1, 1)
        sum_s[here, :] = jnp.where(f == 0, term, sum_s[here, :] + term)

    @pl.when(f == pl.num_programs(0) - 1)
    def _():
        for at in range(0, b_ref.shape[0], ROWS):
            here = slice(at, at + ROWS)
            back = _norm_back(sum_s[here, :].astype(BF16).astype(F32), h_ref[here, :].astype(F32))
            dh2 = (dh_ref[here, :].astype(F32) + back.astype(F32)).astype(BF16)
            dh2_ref[here, :] = dh2
            do_ref[here, :] = _dot(dh2, wo_ref[0], 1, 1).astype(BF16)


def up_back(dg, du, b, h, dh, wg, wu, wo, n, number):
    t, d = b.shape
    ff, width = wg.shape[2], wo.shape[1]
    up, _ = _tiles(d, number)
    whole = ((t, d), lambda i: (0, 0), True)
    hidden = ((t, TILE), lambda i: (0, i))
    return _call(_up_back, "up_back", (ff // TILE,), [hidden, hidden, whole, whole, whole, up, up, ((1, width, d), lambda i: (number, 0, 0), True)],
                 [((n, 2, d // n, TILE), lambda i: (0, 0, 0, i), (n, 2, d // n, ff), BF16), ((t, d), lambda i: (0, 0), (t, d), BF16),
                  ((t, width), lambda i: (0, 0), (t, width), BF16)],
                 [pltpu.VMEM((d, t), BF16), pltpu.VMEM((t, d), F32)], 8 * t * d * ff, (dg, du, b, h, dh, wg, wu, wo))


def _qkv_back(a_ref, dq_ref, dk_ref, dv_ref, o_ref, dh2_ref, *rest, further):
    if further:
        h_ref, wq_ref, wk_ref, wv_ref, dw_ref, dh_ref, sum_s = rest
    else:
        dw_ref, sum_s = rest
    f = pl.program_id(0)
    n = dw_ref.shape[0]
    at, ot = a_ref[...].T, o_ref[...].T
    for i, (x, ref) in enumerate(((at, dq_ref), (at, dk_ref), (at, dv_ref), (ot, dh2_ref))):
        term = _dot(x, ref[...])
        sum_s[i] = jnp.where(f == 0, term, sum_s[i] + term)
    if further:
        by = _dot(dq_ref[...], wq_ref[0], 1, 1) + _dot(dk_ref[...], wk_ref[0], 1, 1) + _dot(dv_ref[...], wv_ref[0], 1, 1)
        back = _norm_back(by.astype(BF16).astype(F32), h_ref[...].astype(F32))
        dh_ref[...] = (dh2_ref[...].astype(F32) + back.astype(F32)).astype(BF16)

    @pl.when(f == pl.num_programs(0) - 1)
    def _():
        for i in range(4):
            dw_ref[:, i] = sum_s[i].astype(BF16).reshape(n, -1, dw_ref.shape[3])


def qkv_back(a, dq, dk, dv, o, dh2, h, wq, wk, wv, n, number):
    t, d = a.shape
    width = dq.shape[1]
    rows = ((ROWS, d), lambda i: (i, 0))
    w = ((1, d, width), lambda i: (number, 0, 0), True)
    ins, outs, args = [rows] * 6, [((n, 4, d // n, width), lambda i: (0, 0, 0, 0), (n, 4, d // n, width), BF16)], (a, dq, dk, dv, o, dh2)
    further = number > 0
    if further:
        ins, outs, args = ins + [rows, w, w, w], outs + [(*rows, (t, d), BF16)], (*args, h, wq, wk, wv)
    return _call(functools.partial(_qkv_back, further=further), "qkv_back", (t // ROWS,), ins, outs, [pltpu.VMEM((4, d, width), F32)],
                 (14 if further else 8) * t * d * width, args)


def adamw(w, m, v, g):
    m = 0.9 * m + 0.1 * g
    v = 0.95 * v + 0.05 * g * g
    step = m * lax.rsqrt(v + 1e-8) + 0.1 * w
    return (w - 0.02 * step).astype(BF16), m, v


def solution(mesh):
    n = mesh.shape["dp"]

    def scattered(x):
        return lax.psum_scatter(x, "dp", scatter_dimension=0, tiled=True)

    def step(x, dy, *arrays):
        weights, m, v = (arrays[i : i + 7] for i in (0, 7, 14))
        wq, wk, wv, wo, wg, wu, wd = weights
        layers, d = wq.shape[:2]
        t = x.shape[1]
        angle = jnp.arange(t, dtype=F32)[:, None] * THETA ** (-jnp.arange(HALF, dtype=F32) / HALF)
        cos, sin = jnp.cos(angle), jnp.sin(angle)
        h, kept = x[0], []
        for number in range(layers):
            a, q, k, v_ = qkv(h, wq, wk, wv, cos, sin, number)
            o, lse = attend(q, k, v_)
            h2, b = out_and_norm(h, o, wo, number)
            last = number == layers - 1
            hidden = (b,)
            if not last:
                *hidden, after = mlp(b, h2, wg, wu, wd, number)
            kept.append((h, a, q, k, v_, o, lse, h2, b, hidden))
            h = None if last else after
        by_h, mine, ends = dy[0], [None] * layers, []
        squares = jnp.zeros((), F32)

        def sums(x):
            ends.append(scattered(x))

        def waited(x):
            nonlocal squares
            done, squares, x = lax.optimization_barrier((ends.pop(0), squares, x))
            squares = squares + jnp.sum(jnp.square(done.astype(F32)))
            got.append(done)
            return x

        got = []
        for number in reversed(range(layers)):
            h, a, q, k, v_, o, lse, h2, b, hidden = kept[number]
            dg, du, by_down = mlp_back(hidden, by_h, wg, wu, wd, number)
            sums(by_down)
            if len(ends) > 2:
                dg = waited(dg)
            by_up, by_h2, by_o = up_back(dg, du, b, h2, by_h, wg, wu, wo, n, number)
            sums(by_up)
            by_o = waited(by_o)
            dq, dk, dv = attend_back(q, k, v_, by_o, o, lse, cos, sin)
            if len(ends) > 1:
                dq = waited(dq)
            by_attention, *by_h = qkv_back(a, dq, dk, dv, o, by_h2, h, wq, wk, wv, n, number)
            by_h = by_h[0] if by_h else None
            sums(by_attention)
        while ends:
            waited(jnp.zeros((), F32))
        for number in range(layers):
            by_down, by_up, by_attention = got[3 * (layers - 1 - number) :][:3]
            mine[number] = [*(by_attention[0, i] for i in range(4)), by_up[0, 0], by_up[0, 1], by_down]
        gradients = [[one[i].astype(F32) for one in mine] for i in range(7)]
        squares = lax.psum(squares, "dp")
        factor = jnp.minimum(1.0, 0.5 * lax.rsqrt(squares / (n * sum(one.size for one in m)) + 1e-30))
        me = lax.axis_index("dp")
        new, whole, sent = [None] * 7, [None] * 7, []
        for group in ((4, 5), (6,), (0, 1, 2, 3)):
            for i in group:
                m_, v_, per = m[i], v[i], gradients[i]
                own = lax.dynamic_slice_in_dim(weights[i], me * m_.shape[1], m_.shape[1], 1).astype(F32)
                if sent:
                    sent[-1], own = lax.optimization_barrier((sent[-1], own))
                new[i] = adamw(own, m_, v_, jnp.stack(per) * factor)
            sent.append(jnp.stack([new[i][0] for i in group]))
        before = None
        for group, one in zip(((4, 5), (6,), (0, 1, 2, 3)), sent):
            got = lax.all_gather(one, "dp")
            if before is not None:
                got, before = lax.optimization_barrier((got, before))
                for i, w in zip(last_group, before):
                    whole[i] = w
            for place, i in enumerate(group):
                whole[i] = got[:, place].transpose(1, 0, 2, 3).reshape(weights[i].shape)
            before, last_group = [whole[i] for i in group], group
        return (*whole, *(one[1] for one in new), *(one[2] for one in new))

    states, all_of, cut = P(("rep", "dp"), None, None), P(None, None, None), P(None, "dp", None)
    return jax.shard_map(
        step,
        mesh=mesh,
        in_specs=(states, states) + (all_of,) * 7 + (cut,) * 14,
        out_specs=(P("rep", None, None),) * 7 + (P("rep", "dp", None),) * 14,
        check_vma=False,
    )
```

```python
import functools

import jax
import jax.numpy as jnp
import numpy as np
from jax import lax
from jax.experimental import pallas as pl
from jax.experimental.pallas import tpu as pltpu
from jax.sharding import PartitionSpec as P

NEG = -1e30
HIDDEN = 2 * NEG
LOG2E = 1.4426950408889634
VMEM = 63 * 2**20
HEAD = 256
HALF = HEAD // 2
THETA = 10000
NAMES = ("wq", "wk", "wv", "wo", "w_gate", "w_up", "w_down")
F32, BF16 = jnp.float32, jnp.bfloat16


def _dot(a, b, ca=1, cb=0):
    return lax.dot_general(a, b, (((ca,), (cb,)), ((), ())), preferred_element_type=F32)


def _call(kernel, name, grid, ins, outs, scratch, flops, args):
    def spec(block, index, still=False):
        return pl.BlockSpec(block, index, pipeline_mode=pl.Buffered(1)) if still else pl.BlockSpec(block, index)

    shapes = [jax.ShapeDtypeStruct(o[2], o[3]) for o in outs]
    moved = sum(a.size * a.dtype.itemsize for a in (*args, *shapes))
    return pl.pallas_call(
        kernel,
        name=name,
        grid=grid,
        in_specs=[spec(*i) for i in ins],
        out_specs=[spec(o[0], o[1]) for o in outs],
        out_shape=shapes,
        scratch_shapes=scratch,
        compiler_params=pltpu.CompilerParams(dimension_semantics=("arbitrary",) * len(grid), vmem_limit_bytes=VMEM),
        cost_estimate=pl.CostEstimate(flops=flops, transcendentals=0, bytes_accessed=moved),
    )(*args)


def _still(*shape):
    return shape, lambda *i: (0,) * len(shape), True


def _of_layer(number, *shape):
    return (1, *shape), lambda i: (number, 0, 0), True


def _row(*shape):
    return shape, lambda i: (i, 0)


def _col(*shape):
    return shape, lambda i: (0, i)


def _mask(bk, wide, shift):
    return lax.broadcasted_iota(jnp.int32, (bk, wide), 1) + shift >= lax.broadcasted_iota(jnp.int32, (bk, wide), 0)


def _cols(i):
    return slice(i * HEAD, (i + 1) * HEAD)


def _attend(q_ref, k_ref, v_ref, o_ref, lse_ref, top_s, mix_s, *, scale, bq, bk, heads):
    iq = pl.program_id(1)
    e = scale * LOG2E
    wide = bk
    top_s[...] = jnp.full(top_s.shape, NEG, F32)
    mix_s[...] = jnp.zeros(mix_s.shape, F32)
    ones = jnp.ones((8, bk), BF16)

    def block(j, strips):
        here = pl.ds(pl.multiple_of(j * bk, bk), bk)
        pieces = [(i, at, cut) for i in range(heads) for at, cut in strips]
        scores = [_dot(k_ref[here, _cols(i)], q_ref[at : at + wide, _cols(i)], 1, 1) for i, at, _ in pieces]
        weights, keeps = [], []
        for (i, at, cut), s in zip(pieces, scores):
            if cut:
                s = jnp.where(_mask(bk, wide, 0), s, HIDDEN)
            old = top_s[i : i + 1, at : at + wide]
            top = jnp.maximum(old, s.max(axis=0, keepdims=True))
            top_s[i : i + 1, at : at + wide] = top
            weights.append(jnp.exp2((s - top) * e).astype(BF16))
            keeps.append(jnp.exp2((old - top) * e))
        for (i, at, _), p, keep in zip(pieces, weights, keeps):
            values = jnp.concatenate([v_ref[here, _cols(i)].T, ones], axis=0)
            mix_s[i, :, at : at + wide] = mix_s[i, :, at : at + wide] * keep + _dot(values, p)

    n = bq // bk
    lax.fori_loop(0, iq * n, lambda j, _: block(j, [(at, False) for at in range(0, bq, wide)]), None)
    for d in range(n):
        block(iq * n + d, [(at, at == d * bk) for at in range(d * bk, bq, wide)])
    for i in range(heads):
        top, total = top_s[i : i + 1, :], mix_s[i, HEAD : HEAD + 1, :]
        o_ref[:, _cols(i)] = (mix_s[i, :HEAD, :] * (1 / total)).T.astype(BF16)
        lse_ref[i : i + 1, :] = top * scale + jnp.log(total)


def attend(q, k, v):
    t, width = q.shape
    heads, bq, bk = width // HEAD, min(1024, t), min(512, t)
    return _call(
        functools.partial(_attend, scale=HEAD**-0.5, bq=bq, bk=bk, heads=heads),
        "attend",
        (1, t // bq),
        [((bq, width), lambda ih, iq: (iq, 0)), ((t, width), lambda ih, iq: (0, 0), True), ((t, width), lambda ih, iq: (0, 0), True)],
        [((bq, width), lambda ih, iq: (iq, 0), (t, width), BF16), ((heads, bq), lambda ih, iq: (0, iq), (heads, t), F32)],
        [pltpu.VMEM((heads, bq), F32), pltpu.VMEM((heads, HEAD + 8, bq), F32)],
        2 * t * t * width,
        (q, k, v),
    )


def _turn(x, cos, sin, back=False):
    a, b = x[:, :HALF], x[:, HALF:]
    if back:
        return jnp.concatenate([a * cos + b * sin, b * cos - a * sin], axis=1)
    return jnp.concatenate([a * cos - b * sin, b * cos + a * sin], axis=1)


def _attend_back(q_ref, k_ref, v_ref, do_ref, o_ref, lse_ref, cosq_ref, sinq_ref, cos_ref, sin_ref, dq_ref, dk_ref, dv_ref, dq_s, dk_s, dv_s,
                 delta_s, lse_s, *, scale, bq, bk, heads):
    ih, iq = pl.program_id(0), pl.program_id(1)
    e = scale * LOG2E
    wide = bk

    @pl.when(iq == 0)
    def _():
        dk_s[...] = jnp.zeros_like(dk_s)
        dv_s[...] = jnp.zeros_like(dv_s)

    dq_s[...] = jnp.zeros_like(dq_s)
    for i in range(heads):
        delta_s[i : i + 1, :] = (do_ref[:, _cols(i)].astype(F32) * o_ref[:, _cols(i)].astype(F32)).T.sum(axis=0, keepdims=True)
        lse_s[i : i + 1, :] = lse_ref[0, i : i + 1, :] * LOG2E

    def block(j, strips):
        here = pl.ds(pl.multiple_of(j * bk, bk), bk)
        pieces = [(i, at, cut) for i in range(heads) for at, cut in strips]
        qs = [q_ref[at : at + wide, _cols(i)] for i, at, _ in pieces]
        dos = [do_ref[at : at + wide, _cols(i)] for i, at, _ in pieces]
        scores = [_dot(k_ref[here, _cols(i)], x, 1, 1) for (i, _, _), x in zip(pieces, qs)]
        dps = [_dot(v_ref[here, _cols(i)], x, 1, 1) for (i, _, _), x in zip(pieces, dos)]
        for n, (i, at, cut) in enumerate(pieces):
            p = jnp.exp2(scores[n] * e - lse_s[i : i + 1, at : at + wide])
            if cut:
                p = jnp.where(_mask(bk, wide, 0), p, 0.0)
            ds = (p * (dps[n] - delta_s[i : i + 1, at : at + wide])).astype(BF16)
            dv_s[i, here, :] += _dot(p.astype(BF16), dos[n])
            dk_s[i, here, :] += _dot(ds, qs[n])
            dq_s[i, :, at : at + wide] += _dot(k_ref[here, _cols(i)].T, ds)

    n = bq // bk
    lax.fori_loop(0, iq * n, lambda j, _: block(j, [(at, False) for at in range(0, bq, wide)]), None)
    for d in range(n):
        block(iq * n + d, [(at, at == d * bk) for at in range(d * bk, bq, wide)])
    for i in range(heads):
        dq_ref[:, _cols(i)] = _turn((dq_s[i] * scale).T.astype(BF16).astype(F32), cosq_ref[...], sinq_ref[...], True).astype(BF16)

    @pl.when(iq == pl.num_programs(1) - 1)
    def _():
        for i in range(heads):
            dk_ref[:, _cols(i)] = _turn((dk_s[i] * scale).astype(BF16).astype(F32), cos_ref[...], sin_ref[...], True).astype(BF16)
            dv_ref[:, _cols(i)] = dv_s[i].astype(BF16)


def attend_back(q, k, v, d_out, out, lse, cos, sin):
    t, width = q.shape
    heads, bq, bk = 2, min(1024, t), min(512, t)
    cols = heads * HEAD
    queries = ((bq, cols), lambda ih, iq: (iq, ih))
    keys = ((t, cols), lambda ih, iq: (0, ih))
    stats = ((1, heads, bq), lambda ih, iq: (ih, 0, iq))
    table_q = ((bq, HALF), lambda ih, iq: (iq, 0))
    table = ((t, HALF), lambda ih, iq: (0, 0), True)
    return _call(
        functools.partial(_attend_back, scale=HEAD**-0.5, bq=bq, bk=bk, heads=heads),
        "attend_back",
        (width // cols, t // bq),
        [queries, keys, keys, queries, queries, stats, table_q, table_q, table, table],
        [(*queries, (t, width), BF16), (*keys, (t, width), BF16), (*keys, (t, width), BF16)],
        [pltpu.VMEM((heads, HEAD, bq), F32), pltpu.VMEM((heads, t, HEAD), F32), pltpu.VMEM((heads, t, HEAD), F32),
         pltpu.VMEM((heads, bq), F32), pltpu.VMEM((heads, bq), F32)],
        5 * t * t * width,
        (q, k, v, d_out, out, lse.reshape(-1, heads, t), cos, sin, cos, sin),
    )


ROWS = 512
BLOCK = 512
PIECE = 512
TILE = 512


def _chunks(size, body):
    for at in range(0, size, ROWS):
        body(slice(at, at + ROWS))


def _scale_of(h):
    return lax.rsqrt(jnp.mean(h * h, axis=-1, keepdims=True) + 1e-6)


def _norm(h):
    return (h * _scale_of(h)).astype(BF16)


def _norm_back(by, h):
    r = _scale_of(h)
    return (by * r - h * (r * r * r * jnp.mean(by * h, axis=-1, keepdims=True))).astype(BF16)


def _qkv(h_ref, wq_ref, wk_ref, wv_ref, cos_ref, sin_ref, at_ref, q_ref, k_ref, v_ref):
    a = _norm(h_ref[...].astype(F32))
    at_ref[...] = a.T
    cos, sin = cos_ref[...], sin_ref[...]
    width = q_ref.shape[1]
    for at in range(0, width, PIECE):
        for w_ref, to_ref in ((wq_ref, q_ref), (wk_ref, k_ref)):
            t = _dot(a, w_ref[0, :, at : at + PIECE])
            for i in range(PIECE // HEAD):
                one = _turn(t[:, _cols(i)].astype(BF16).astype(F32), cos, sin)
                to_ref[:, at + i * HEAD : at + (i + 1) * HEAD] = one.astype(BF16)
        v_ref[:, at : at + PIECE] = _dot(a, wv_ref[0, :, at : at + PIECE]).astype(BF16)


def qkv(h, wq, wk, wv, cos, sin, number):
    t, d = h.shape
    width = wq.shape[2]
    rows = _row(BLOCK, d)
    wide = _row(BLOCK, width)
    w = _of_layer(number, d, width)
    table = _row(BLOCK, HALF)
    return _call(_qkv, "qkv", (t // BLOCK,), [rows, w, w, w, table, table],
                 [((d, BLOCK), lambda i: (0, i), (d, t), BF16)] + [(*wide, (t, width), BF16)] * 3, [], 6 * t * d * width, (h, wq, wk, wv, cos, sin))


def _out(h_ref, o_ref, w_ref, h2_ref, b_ref, bt_ref):
    h2 = (h_ref[...].astype(F32) + _dot(o_ref[...], w_ref[0]).astype(BF16).astype(F32)).astype(BF16)
    h2_ref[...] = h2
    b = _norm(h2.astype(F32))
    b_ref[...] = b
    bt_ref[...] = b.T


def out_and_norm(h, o, wo, number):
    t, d = h.shape
    width = o.shape[1]
    rows, wide = _row(BLOCK, d), _row(BLOCK, width)
    return _call(_out, "out", (t // BLOCK,), [rows, wide, _of_layer(number, width, d)],
                 [(*rows, (t, d), BF16)] * 2 + [((d, BLOCK), lambda i: (0, i), (d, t), BF16)], [], 2 * t * d * width, (h, o, wo))


def _mlp(b_ref, h_ref, wg_ref, wu_ref, wd_ref, g_ref, u_ref, to_ref, sum_s):
    f = pl.program_id(0)

    @pl.when(f == 0)
    def _():
        sum_s[...] = jnp.zeros_like(sum_s)

    def chunk(here):
        b = b_ref[here, :]
        g, u = _dot(b, wg_ref[0]), _dot(b, wu_ref[0])
        g_ref[here, :], u_ref[here, :] = g, u
        sum_s[here, :] += _dot((g * jax.nn.sigmoid(g) * u).astype(BF16), wd_ref[0])

    _chunks(b_ref.shape[0], chunk)

    @pl.when(f == pl.num_programs(0) - 1)
    def _():
        to_ref[...] = (h_ref[...].astype(F32) + sum_s[...].astype(BF16).astype(F32)).astype(BF16)


def _tiles(d, number):
    up = ((1, d, TILE), lambda i: (number, 0, i))
    down = ((1, TILE, d), lambda i: (number, i, 0))
    return up, down


def mlp(b, h, wg, wu, wd, number):
    t, d = b.shape
    ff = wg.shape[2]
    up, down = _tiles(d, number)
    whole = _still(t, d)
    hidden = _col(t, TILE)
    return _call(_mlp, "mlp", (ff // TILE,), [whole, whole, up, up, down],
                 [(*hidden, (t, ff), F32)] * 2 + [((t, d), lambda i: (0, 0), (t, d), BF16)], [pltpu.VMEM((t, d), F32)], 6 * t * d * ff,
                 (b, h, wg, wu, wd))


def _mlp_back(dh_ref, wd_ref, g_of, u_of, dg_ref, du_ref, dwd_ref, act_s):
    def chunk(here):
        g, u = g_of(here), u_of(here)
        by = _dot(dh_ref[here, :], wd_ref[0], 1, 1).astype(BF16).astype(F32)
        s = jax.nn.sigmoid(g)
        silu = g * s
        act_s[here, :] = (silu * u).astype(BF16)
        du_ref[here, :] = (by * silu).astype(BF16)
        dg_ref[here, :] = (by * u * (s + silu * (1 - s))).astype(BF16)

    _chunks(dh_ref.shape[0], chunk)
    dwd_ref[...] = _dot(act_s[...].T, dh_ref[...]).astype(BF16)


def _mlp_back_anew(b_ref, dh_ref, wg_ref, wu_ref, wd_ref, *rest):
    _mlp_back(dh_ref, wd_ref, lambda here: _dot(b_ref[here, :], wg_ref[0]), lambda here: _dot(b_ref[here, :], wu_ref[0]), *rest)


def _mlp_back_kept(g_ref, u_ref, dh_ref, wd_ref, *rest):
    _mlp_back(dh_ref, wd_ref, lambda here: g_ref[here, :], lambda here: u_ref[here, :], *rest)


def mlp_back(kept, dh, wg, wu, wd, number):
    t, d = dh.shape
    ff = wg.shape[2]
    up, down = _tiles(d, number)
    whole = _still(t, d)
    hidden = _col(t, TILE)
    if len(kept) == 2:
        kernel, ins, args, work = _mlp_back_kept, [hidden, hidden, whole, down], (*kept, dh, wd), 4
    else:
        kernel, ins, args, work = _mlp_back_anew, [whole, whole, up, up, down], (*kept, dh, wg, wu, wd), 8
    return _call(kernel, "mlp_back", (ff // TILE,), ins,
                 [(*hidden, (t, ff), BF16)] * 2 + [((TILE, d), lambda i: (i, 0), (ff, d), BF16)], [pltpu.VMEM((t, TILE), BF16)],
                 work * t * d * ff, args)


def _up_grad(dg_ref, du_ref, bt_ref, dw_ref):
    n, d = dw_ref.shape[0], bt_ref.shape[0]
    for i, ref in enumerate((dg_ref, du_ref)):
        dw_ref[:, i] = _dot(bt_ref[...], ref[...]).astype(BF16).reshape(n, d // n, TILE)


def up_grad(dg, du, bt, n):
    d, t = bt.shape
    ff = dg.shape[1]
    hidden = _col(t, TILE)
    return _call(_up_grad, "up_grad", (ff // TILE,), [hidden, hidden, _still(d, t)],
                 [((n, 2, d // n, TILE), lambda i: (0, 0, 0, i), (n, 2, d // n, ff), BF16)], [], 4 * t * d * ff, (dg, du, bt))[0]


def _up_back(dg_ref, du_ref, h_ref, dh_ref, wg_ref, wu_ref, wo_ref, dh2_ref, do_ref, sum_s):
    f = pl.program_id(0)

    @pl.when(f == 0)
    def _():
        sum_s[...] = jnp.zeros_like(sum_s)

    def chunk(here):
        sum_s[here, :] += _dot(dg_ref[here, :], wg_ref[0], 1, 1) + _dot(du_ref[here, :], wu_ref[0], 1, 1)

    _chunks(h_ref.shape[0], chunk)

    def last(here):
        back = _norm_back(sum_s[here, :].astype(BF16).astype(F32), h_ref[here, :].astype(F32))
        dh2 = (dh_ref[here, :].astype(F32) + back.astype(F32)).astype(BF16)
        dh2_ref[here, :] = dh2
        do_ref[here, :] = _dot(dh2, wo_ref[0], 1, 1).astype(BF16)

    @pl.when(f == pl.num_programs(0) - 1)
    def _():
        _chunks(h_ref.shape[0], last)


def up_back(dg, du, h, dh, wg, wu, wo, number):
    t, d = h.shape
    ff, width = wg.shape[2], wo.shape[1]
    up, _ = _tiles(d, number)
    whole = _still(t, d)
    hidden = _col(t, TILE)
    return _call(_up_back, "up_back", (ff // TILE,), [hidden, hidden, whole, whole, up, up, _of_layer(number, width, d)],
                 [((t, d), lambda i: (0, 0), (t, d), BF16), ((t, width), lambda i: (0, 0), (t, width), BF16)],
                 [pltpu.VMEM((t, d), F32)], 4 * t * d * ff, (dg, du, h, dh, wg, wu, wo))


def _qkv_back(at_ref, dq_ref, dk_ref, dv_ref, o_ref, dh2_ref, *rest, further):
    if further:
        h_ref, wq_ref, wk_ref, wv_ref, dw_ref, dh_ref, sum_s = rest
    else:
        dw_ref, sum_s = rest
    f = pl.program_id(0)
    n = dw_ref.shape[0]
    at, ot = at_ref[...], o_ref[...].T
    for i, (x, ref) in enumerate(((at, dq_ref), (at, dk_ref), (at, dv_ref), (ot, dh2_ref))):
        term = _dot(x, ref[...])
        sum_s[i] = jnp.where(f == 0, term, sum_s[i] + term)
    if further:
        by = _dot(dq_ref[...], wq_ref[0], 1, 1) + _dot(dk_ref[...], wk_ref[0], 1, 1) + _dot(dv_ref[...], wv_ref[0], 1, 1)
        back = _norm_back(by.astype(BF16).astype(F32), h_ref[...].astype(F32))
        dh_ref[...] = (dh2_ref[...].astype(F32) + back.astype(F32)).astype(BF16)

    @pl.when(f == pl.num_programs(0) - 1)
    def _():
        for i in range(4):
            dw_ref[:, i] = sum_s[i].astype(BF16).reshape(n, -1, dw_ref.shape[3])


def qkv_back(at, dq, dk, dv, o, dh2, h, wq, wk, wv, n, number):
    d, t = at.shape
    width = dq.shape[1]
    rows = _row(BLOCK, d)
    w = _of_layer(number, d, width)
    ins, outs, args = [_col(d, BLOCK)] + [rows] * 5, [((n, 4, d // n, width), lambda i: (0, 0, 0, 0), (n, 4, d // n, width), BF16)], (at, dq, dk, dv, o, dh2)
    further = number > 0
    if further:
        ins, outs, args = ins + [rows, w, w, w], outs + [(*rows, (t, d), BF16)], (*args, h, wq, wk, wv)
    return _call(functools.partial(_qkv_back, further=further), "qkv_back", (t // BLOCK,), ins, outs, [pltpu.VMEM((4, d, width), F32)],
                 (14 if further else 8) * t * d * width, args)


def _places(layout):
    me = lax.axis_index("dp")
    x, y, core = lax.div(me, 4), lax.rem(lax.div(me, 2), 2), lax.rem(me, 2)
    place = lambda x, y, core: layout(x, y, core)
    return core, place(x, y, core), place(1 - x, y, core), place(x, 1 - y, core), place(1 - x, 1 - y, core), place(x, y, 1 - core)


def _device(x, y, core):
    return x * 4 + y * 2 + core


def _chip(x, y, core):
    return x * 2 + y


def _meet(*peers):
    barrier = pltpu.get_barrier_semaphore()
    for peer in peers:
        pl.semaphore_signal(barrier, inc=1, device_id={"dp": peer}, device_id_type=pl.DeviceIdType.MESH)
    pl.semaphore_wait(barrier, len(peers))


def _scatter(x_ref, *refs, early):
    early_refs, (out_ref, squares_ref, core_s, to_x_s, to_y_s, from_x_s, from_y_s, on_y_s, on_x_s, last_y_s, last_x_s, send_sem, recv_sem) = (
        refs[:early], refs[early:])
    core, me, across_x, across_y, _, partner = _places(_device)
    _, chip, chip_x, chip_y, chip_d, _ = _places(_chip)
    _meet(across_x, across_y, partner)

    def send(i, src, dst, peer):
        copy = pltpu.make_async_remote_copy(src_ref=src, dst_ref=dst, send_sem=send_sem.at[i], recv_sem=recv_sem.at[i],
                                            device_id={"dp": peer}, device_id_type=pl.DeviceIdType.MESH)
        copy.start()
        return copy

    order = (chip_d, chip_x, chip_y, chip)
    swaps = [send(i, x_ref.at[to, 1 - core], core_s.at[to], partner) for i, to in enumerate(order)]
    first, second = slice(0, 2), slice(2, 4)

    def on_chip(to, half):
        return x_ref[to, core, half].astype(F32) + core_s[to, half].astype(F32)

    swaps[0].wait()
    to_x_s[1], to_y_s[1] = on_chip(chip_d, first).astype(BF16), on_chip(chip_d, second).astype(BF16)
    swaps[1].wait()
    to_x_s[0] = on_chip(chip_x, first).astype(BF16)
    swaps[2].wait()
    to_y_s[0] = on_chip(chip_y, second).astype(BF16)
    swaps[3].wait()
    by_x, by_y = send(4, to_x_s, from_x_s, across_x), send(5, to_y_s, from_y_s, across_y)
    squares = jnp.zeros((), F32)
    for ref in early_refs:
        squares += jnp.sum(jnp.square(ref[...].astype(F32)))
    by_x.wait()
    on_y_s[...] = (on_chip(chip_y, first) + from_x_s[1].astype(F32)).astype(BF16)
    by_y.wait()
    on_x_s[...] = (on_chip(chip_x, second) + from_y_s[1].astype(F32)).astype(BF16)
    then_y, then_x = send(6, on_y_s, last_y_s, across_y), send(7, on_x_s, last_x_s, across_x)
    for copy, half, came, last in ((then_y, first, from_x_s, last_y_s), (then_x, second, from_y_s, last_x_s)):
        copy.wait()
        done = (on_chip(chip, half) + came[0].astype(F32) + last[...].astype(F32)).astype(BF16)
        out_ref[0, half] = done
        squares += jnp.sum(jnp.square(done.astype(F32)))
    squares_ref[...] = jnp.full(squares_ref.shape, squares)


def scatter(x, early):
    n, four, rows, cols = x.shape
    half = pltpu.VMEM((2, rows, cols), BF16)
    pair = pltpu.VMEM((2, 2, rows, cols), BF16)
    vmem = pl.BlockSpec(memory_space=pltpu.VMEM)
    return pl.pallas_call(
        functools.partial(_scatter, early=len(early)),
        name="scatter",
        in_specs=[vmem] * (1 + len(early)),
        out_specs=[vmem, vmem],
        out_shape=[jax.ShapeDtypeStruct((1, four, rows, cols), BF16), jax.ShapeDtypeStruct((8, 128), F32)],
        scratch_shapes=[pltpu.VMEM((4, four, rows, cols), BF16), pair, pair, pair, pair, half, half, half, half,
                        pltpu.SemaphoreType.DMA((8,)), pltpu.SemaphoreType.DMA((8,))],
        compiler_params=pltpu.CompilerParams(collective_id=1, has_side_effects=True, vmem_limit_bytes=VMEM),
        cost_estimate=pl.CostEstimate(flops=2**34, transcendentals=0, bytes_accessed=2 * x.size),
    )(x.reshape(4, 2, four, rows, cols), *early)


def _gather(*refs, count):
    x_refs, out_refs, (own_sem, send_sem, recv_sem) = refs[:count], refs[count : 2 * count], refs[2 * count :]
    _, me, across_x, across_y, across, partner = _places(_device)
    _meet(across_x, across_y, partner)
    owns = [pltpu.make_async_copy(x_ref, out_ref.at[me], own_sem.at[i]) for i, (x_ref, out_ref) in enumerate(zip(x_refs, out_refs))]
    for own in owns:
        own.start()
    sent = []

    def send(i, src, dst, peer):
        at = len(sent)
        copy = pltpu.make_async_remote_copy(src_ref=src, dst_ref=dst, send_sem=send_sem.at[at], recv_sem=recv_sem.at[at],
                                            device_id={"dp": peer}, device_id_type=pl.DeviceIdType.MESH)
        copy.start()
        sent.append(copy)
        return copy

    def pass_on(i, device, peer, half=None):
        block = out_refs[i].at[device] if half is None else out_refs[i].at[device, half]
        return send(i, block, block, peer)

    each = range(count)
    halves = [(slice(0, ref.shape[0] // 2), slice(ref.shape[0] // 2, ref.shape[0])) for ref in x_refs]
    to_x = [send(i, x_refs[i], out_refs[i].at[me], across_x) for i in each]
    to_y = [send(i, x_refs[i], out_refs[i].at[me], across_y) for i in each]
    to_core = [send(i, x_refs[i], out_refs[i].at[me], partner) for i in each]
    on_y, on_x = [], []
    for i in each:
        to_x[i].wait_recv()
        on_y.append(pass_on(i, across_x, across_y, halves[i][0]))
        to_core.append(pass_on(i, across_x, partner))
        to_y[i].wait_recv()
        on_x.append(pass_on(i, across_y, across_x, halves[i][1]))
        to_core.append(pass_on(i, across_y, partner))
    for i in each:
        on_y[i].wait_recv()
        to_core.append(pass_on(i, across, partner, halves[i][0]))
        on_x[i].wait_recv()
        to_core.append(pass_on(i, across, partner, halves[i][1]))
    for copy in to_core:
        copy.wait_recv()
    for copy in sent:
        copy.wait_send()
    for own in owns:
        own.wait()


def gather(*xs):
    anywhere = pl.BlockSpec(memory_space=pl.ANY)
    count = len(xs)
    sems = pltpu.SemaphoreType.DMA((9 * count,))
    return pl.pallas_call(
        functools.partial(_gather, count=count),
        name="gather",
        in_specs=[anywhere] * count,
        out_specs=[anywhere] * count,
        out_shape=[jax.ShapeDtypeStruct((8, *x.shape), x.dtype) for x in xs],
        scratch_shapes=[pltpu.SemaphoreType.DMA((count,)), sems, sems],
        compiler_params=pltpu.CompilerParams(collective_id=2, has_side_effects=True, vmem_limit_bytes=VMEM),
        cost_estimate=pl.CostEstimate(flops=2**34, transcendentals=0, bytes_accessed=2**25),
    )(*xs)


def _total(x_ref, sum_ref, got_s, send_sem, recv_sem, *, n):
    me = lax.axis_index("dp")
    peers = [lax.rem(me + k, n) for k in range(1, n)]
    barrier = pltpu.get_barrier_semaphore()
    for peer in peers:
        pl.semaphore_signal(barrier, inc=1, device_id={"dp": peer}, device_id_type=pl.DeviceIdType.MESH)
    pl.semaphore_wait(barrier, n - 1)
    copies = []
    for k, peer in enumerate(peers):
        copies.append(pltpu.make_async_remote_copy(src_ref=x_ref, dst_ref=got_s.at[k], send_sem=send_sem.at[k], recv_sem=recv_sem.at[k],
                                                   device_id={"dp": peer}, device_id_type=pl.DeviceIdType.MESH))
        copies[-1].start()
    for copy in copies:
        copy.wait()
    total = jnp.zeros(x_ref.shape, F32)
    for device in range(n):
        one = x_ref[...]
        for k in range(n - 1):
            one = jnp.where(lax.rem(me + n - k - 1, n) == device, got_s[k], one)
        total = total + one
    sum_ref[...] = total


def total(x, n):
    shape = (8, 128)
    return pl.pallas_call(
        functools.partial(_total, n=n),
        name="total",
        in_specs=[pl.BlockSpec(memory_space=pltpu.VMEM)],
        out_specs=pl.BlockSpec(memory_space=pltpu.VMEM),
        out_shape=jax.ShapeDtypeStruct(shape, F32),
        scratch_shapes=[pltpu.VMEM((n - 1, *shape), F32), pltpu.SemaphoreType.DMA((n - 1,)), pltpu.SemaphoreType.DMA((n - 1,))],
        compiler_params=pltpu.CompilerParams(collective_id=0, has_side_effects=True),
    )(jnp.full(shape, x))


def _adamw(me_ref, squares_ref, *refs, count, size):
    ws, ms, vs, refs = refs[:count], refs[count : 2 * count], refs[2 * count : 3 * count], refs[3 * count :]
    layers = ws[0].shape[0]
    grads, refs = refs[:layers], refs[layers:]
    sents, refs = (refs[:1], refs[1:]) if count > 1 else (refs[:layers], refs[layers:])
    new_ms, new_vs = refs[:count], refs[count:]
    factor = jnp.minimum(1.0, 0.5 * lax.rsqrt(squares_ref[0:1, 0:1] / size + 1e-30))
    for i in range(count):
        for layer in range(layers):
            g = (grads[layer][0, i] if count > 1 else grads[layer][...]).astype(F32) * factor
            m = 0.9 * ms[i][layer] + 0.1 * g
            v = 0.95 * vs[i][layer] + 0.05 * g * g
            w = ws[i][layer].astype(F32)
            new_ms[i][layer], new_vs[i][layer] = m, v
            to = sents[0].at[i, layer] if count > 1 else sents[layer]
            to[...] = (w - 0.02 * (m * lax.rsqrt(v + 1e-8) + 0.1 * w)).astype(BF16)


def adamw(me, squares, ws, ms, vs, grads, size, tile):
    count = len(ws)
    layers, rows, cols = ms[0].shape
    if count > 1:
        steps, block = cols // tile, (layers, rows, tile)
        mine = lambda i, me: (0, 0, i)
        theirs = lambda i, me: (0, me[0], i)
        grad = pl.BlockSpec((1, count, rows, tile), lambda i, me: (0, 0, 0, i))
        outs = [pl.BlockSpec((count, layers, rows, tile), lambda i, me: (0, 0, 0, i))]
        sent_shape = (count, *ms[0].shape)
    else:
        steps, block = rows // tile, (layers, tile, cols)
        mine = lambda i, me: (0, i, 0)
        theirs = lambda i, me: (0, me[0] * (rows // tile) + i, 0)
        grad = pl.BlockSpec((tile, cols), lambda i, me: (i, 0))
        outs = [grad] * layers
        sent_shape = (rows, cols)
    moment, weight = pl.BlockSpec(block, mine), pl.BlockSpec(block, theirs)
    shape = jax.ShapeDtypeStruct(ms[0].shape, F32)
    many = len(outs)
    got = pl.pallas_call(
        functools.partial(_adamw, count=count, size=size),
        name="adamw",
        grid_spec=pltpu.PrefetchScalarGridSpec(
            num_scalar_prefetch=1,
            grid=(steps,),
            in_specs=[pl.BlockSpec((8, 128), lambda i, me: (0, 0))] + [weight] * count + [moment] * (2 * count) + [grad] * layers,
            out_specs=outs + [moment] * (2 * count),
        ),
        out_shape=[jax.ShapeDtypeStruct(sent_shape, BF16)] * many + [shape] * (2 * count),
        compiler_params=pltpu.CompilerParams(dimension_semantics=("arbitrary",), vmem_limit_bytes=VMEM),
        cost_estimate=pl.CostEstimate(flops=20 * count * ms[0].size, transcendentals=0, bytes_accessed=22 * count * ms[0].size),
    )(me, squares, *ws, *ms, *vs, *grads)
    return got[:many], got[many : many + count], got[many + count :]


def _unpack(got_ref, *w_refs):
    for i, ref in enumerate(w_refs):
        ref[...] = got_ref[0, i]


def unpack(got):
    n, count, layers, rows, cols = got.shape
    return _call(_unpack, "unpack", (n,), [((1, count, layers, rows, cols), lambda i: (i, 0, 0, 0, 0))],
                 [((layers, rows, cols), lambda i: (0, i, 0), (layers, n * rows, cols), BF16)] * count, [], got.size, (got,))


def _place_layer(got_ref, *refs):
    refs[-1][...] = got_ref[...][None]


def place_layer(got, layer, layers, others=None):
    rows, cols = got.size // got.shape[-1], got.shape[-1]
    ins, args = [pl.BlockSpec(*_row(ROWS, cols))], [got.reshape(rows, cols)]
    if others is not None:
        ins, args = ins + [pl.BlockSpec(memory_space=pl.ANY)], args + [others]
    return pl.pallas_call(
        _place_layer,
        name="place_layer",
        grid=(rows // ROWS,),
        in_specs=ins,
        out_specs=pl.BlockSpec((1, ROWS, cols), lambda i: (layer, i, 0)),
        out_shape=jax.ShapeDtypeStruct((layers, rows, cols), got.dtype),
        input_output_aliases={} if others is None else {1: 0},
        compiler_params=pltpu.CompilerParams(dimension_semantics=("arbitrary",), vmem_limit_bytes=VMEM),
        cost_estimate=pl.CostEstimate(flops=got.size, transcendentals=0, bytes_accessed=4 * got.size),
    )(*args)


def solution(mesh):
    n = mesh.shape["dp"]

    def scattered(x):
        return lax.psum_scatter(x, "dp", scatter_dimension=0, tiled=True)

    def step(x, dy, *arrays):
        weights, m, v = (arrays[i : i + 7] for i in (0, 7, 14))
        wq, wk, wv, wo, wg, wu, wd = weights
        layers = wq.shape[0]
        t = x.shape[1]
        angle = np.arange(t, dtype=np.float32)[:, None] * np.float32(THETA) ** (-np.arange(HALF, dtype=np.float32) / np.float32(HALF))
        cos, sin = (jnp.asarray(f(angle.astype(np.float64)).astype(np.float32)) for f in (np.cos, np.sin))
        h, kept = x[0], []
        for number in range(layers):
            at, q, k, v_ = qkv(h, wq, wk, wv, cos, sin, number)
            o, lse = attend(q, k, v_)
            h2, b, bt = out_and_norm(h, o, wo, number)
            last = number == layers - 1
            hidden = (b,)
            if not last:
                *hidden, after = mlp(b, h2, wg, wu, wd, number)
            kept.append((h, at, q, k, v_, o, lse, h2, bt, hidden))
            h = None if last else after
        by_h, ends, got = dy[0], [], []

        def waited(x):
            done, x = lax.optimization_barrier((ends.pop(0), x))
            got.append(done)
            return x

        for number in reversed(range(layers)):
            h, at, q, k, v_, o, lse, h2, bt, hidden = kept[number]
            if ends:
                by_h = waited(by_h)
            dg, du, by_down = mlp_back(hidden, by_h, wg, wu, wd, number)
            ends.append(scattered(by_down))
            by_up = up_grad(dg, du, bt, n)
            if len(ends) > 1:
                dg = waited(dg)
            ends.append(scattered(by_up))
            by_h2, by_o = up_back(dg, du, h2, by_h, wg, wu, wo, number)
            by_o = waited(by_o)
            dq, dk, dv = attend_back(q, k, v_, by_o, o, lse, cos, sin)
            by_attention, *by_h = qkv_back(at, dq, dk, dv, o, by_h2, h, wq, wk, wv, n, number)
            by_h = by_h[0] if by_h else None
            if number > 0:
                ends.append(scattered(by_attention))
        by_attention, squares = scatter(by_attention, got)
        squares = waited(squares)
        squares = squares[0, 0] + jnp.sum(jnp.square(got[-1].astype(F32)))
        got.append(by_attention)
        squares = total(squares, n)
        me = lax.axis_index("dp").astype(jnp.int32)[None]
        size = n * sum(one.size for one in m)
        new_m, new_v, sent = [None] * 7, [None] * 7, []
        groups = (((4, 5), 1, 1024), ((6,), 0, 128), ((0, 1, 2, 3), 2, 512))
        for group, place, tile in groups:
            grads = [got[3 * (layers - 1 - number) + place] for number in range(layers)]
            one, some_m, some_v = adamw(me, squares, *([a[i] for i in group] for a in (weights, m, v)), grads, size, tile)
            one, squares = lax.optimization_barrier((one, squares))
            sent.append(one)
            for i, m_, v_ in zip(group, some_m, some_v):
                new_m[i], new_v[i] = m_, v_
        (up,), (down, last_down), (attention,) = sent
        up, last_down = lax.all_gather(up, "dp"), lax.all_gather(last_down, "dp", tiled=True)
        attention, down = gather(attention, down)
        attention, down = unpack(attention), place_layer(down, 0, layers)
        up, attention, down = lax.optimization_barrier((up, attention, down))
        up = unpack(up)
        last_down, up = lax.optimization_barrier((last_down, up))
        whole = (*attention, *up, place_layer(last_down, layers - 1, layers, down))
        return (*whole, *new_m, *new_v)

    states, all_of, cut = P(("rep", "dp"), None, None), P(None, None, None), P(None, "dp", None)
    return jax.shard_map(
        step,
        mesh=mesh,
        in_specs=(states, states) + (all_of,) * 7 + (cut,) * 14,
        out_specs=(P("rep", None, None),) * 7 + (P("rep", "dp", None),) * 14,
        check_vma=False,
    )
```

```python
import functools

import jax
import jax.numpy as jnp
import numpy as np
from jax import lax
from jax.experimental import pallas as pl
from jax.experimental.pallas import tpu as pltpu
from jax.sharding import PartitionSpec as P

NEG = -1e30
HIDDEN = 2 * NEG
LOG2E = 1.4426950408889634
VMEM = 63 * 2**20
HEAD = 256
HALF = HEAD // 2
THETA = 10000
NAMES = ("wq", "wk", "wv", "wo", "w_gate", "w_up", "w_down")
F32, BF16 = jnp.float32, jnp.bfloat16


def _dot(a, b, ca=1, cb=0):
    return lax.dot_general(a, b, (((ca,), (cb,)), ((), ())), preferred_element_type=F32)


def _call(kernel, name, grid, ins, outs, scratch, flops, args):
    def spec(block, index, still=False):
        return pl.BlockSpec(block, index, pipeline_mode=pl.Buffered(1)) if still else pl.BlockSpec(block, index)

    shapes = [jax.ShapeDtypeStruct(o[2], o[3]) for o in outs]
    moved = sum(a.size * a.dtype.itemsize for a in (*args, *shapes))
    return pl.pallas_call(
        kernel,
        name=name,
        grid=grid,
        in_specs=[spec(*i) for i in ins],
        out_specs=[spec(o[0], o[1]) for o in outs],
        out_shape=shapes,
        scratch_shapes=scratch,
        compiler_params=pltpu.CompilerParams(dimension_semantics=("arbitrary",) * len(grid), vmem_limit_bytes=VMEM),
        cost_estimate=pl.CostEstimate(flops=flops, transcendentals=0, bytes_accessed=moved),
    )(*args)


def _still(*shape):
    return shape, lambda *i: (0,) * len(shape), True


def _of_layer(number, *shape):
    return (1, *shape), lambda i: (number, 0, 0), True


def _row(*shape):
    return shape, lambda i: (i, 0)


def _col(*shape):
    return shape, lambda i: (0, i)


def _mask(bk, wide, shift):
    return lax.broadcasted_iota(jnp.int32, (bk, wide), 1) + shift >= lax.broadcasted_iota(jnp.int32, (bk, wide), 0)


def _cols(i):
    return slice(i * HEAD, (i + 1) * HEAD)


def _attend(q_ref, k_ref, v_ref, o_ref, lse_ref, top_s, mix_s, *, scale, bq, bk, heads):
    iq = pl.program_id(1)
    e = scale * LOG2E
    wide = bk
    top_s[...] = jnp.full(top_s.shape, NEG, F32)
    mix_s[...] = jnp.zeros(mix_s.shape, F32)
    ones = jnp.ones((8, bk), BF16)

    def block(j, strips):
        here = pl.ds(pl.multiple_of(j * bk, bk), bk)
        pieces = [(i, at, cut) for i in range(heads) for at, cut in strips]
        scores = [_dot(k_ref[here, _cols(i)], q_ref[at : at + wide, _cols(i)], 1, 1) for i, at, _ in pieces]
        weights, keeps = [], []
        for (i, at, cut), s in zip(pieces, scores):
            if cut:
                s = jnp.where(_mask(bk, wide, 0), s, HIDDEN)
            old = top_s[i : i + 1, at : at + wide]
            top = jnp.maximum(old, s.max(axis=0, keepdims=True))
            top_s[i : i + 1, at : at + wide] = top
            weights.append(jnp.exp2((s - top) * e).astype(BF16))
            keeps.append(jnp.exp2((old - top) * e))
        for (i, at, _), p, keep in zip(pieces, weights, keeps):
            values = jnp.concatenate([v_ref[here, _cols(i)].T, ones], axis=0)
            mix_s[i, :, at : at + wide] = mix_s[i, :, at : at + wide] * keep + _dot(values, p)

    n = bq // bk
    lax.fori_loop(0, iq * n, lambda j, _: block(j, [(at, False) for at in range(0, bq, wide)]), None)
    for d in range(n):
        block(iq * n + d, [(at, at == d * bk) for at in range(d * bk, bq, wide)])
    for i in range(heads):
        top, total = top_s[i : i + 1, :], mix_s[i, HEAD : HEAD + 1, :]
        o_ref[:, _cols(i)] = (mix_s[i, :HEAD, :] * (1 / total)).T.astype(BF16)
        lse_ref[i : i + 1, :] = top * scale + jnp.log(total)


def attend(q, k, v):
    t, width = q.shape
    heads, bq, bk = width // HEAD, min(1024, t), min(512, t)
    return _call(
        functools.partial(_attend, scale=HEAD**-0.5, bq=bq, bk=bk, heads=heads),
        "attend",
        (1, t // bq),
        [((bq, width), lambda ih, iq: (iq, 0)), ((t, width), lambda ih, iq: (0, 0), True), ((t, width), lambda ih, iq: (0, 0), True)],
        [((bq, width), lambda ih, iq: (iq, 0), (t, width), BF16), ((heads, bq), lambda ih, iq: (0, iq), (heads, t), F32)],
        [pltpu.VMEM((heads, bq), F32), pltpu.VMEM((heads, HEAD + 8, bq), F32)],
        2 * t * t * width,
        (q, k, v),
    )


def _turn(x, cos, sin, back=False):
    a, b = x[:, :HALF], x[:, HALF:]
    if back:
        return jnp.concatenate([a * cos + b * sin, b * cos - a * sin], axis=1)
    return jnp.concatenate([a * cos - b * sin, b * cos + a * sin], axis=1)


def _attend_back(q_ref, k_ref, v_ref, do_ref, o_ref, lse_ref, cosq_ref, sinq_ref, cos_ref, sin_ref, dq_ref, dk_ref, dv_ref, dq_s, dk_s, dv_s,
                 delta_s, lse_s, *, scale, bq, bk, heads):
    ih, iq = pl.program_id(0), pl.program_id(1)
    e = scale * LOG2E
    wide = bk

    @pl.when(iq == 0)
    def _():
        dk_s[...] = jnp.zeros_like(dk_s)
        dv_s[...] = jnp.zeros_like(dv_s)

    dq_s[...] = jnp.zeros_like(dq_s)
    for i in range(heads):
        delta_s[i : i + 1, :] = (do_ref[:, _cols(i)].astype(F32) * o_ref[:, _cols(i)].astype(F32)).T.sum(axis=0, keepdims=True)
        lse_s[i : i + 1, :] = lse_ref[0, i : i + 1, :] * LOG2E

    def block(j, strips):
        here = pl.ds(pl.multiple_of(j * bk, bk), bk)
        pieces = [(i, at, cut) for i in range(heads) for at, cut in strips]
        qs = [q_ref[at : at + wide, _cols(i)] for i, at, _ in pieces]
        dos = [do_ref[at : at + wide, _cols(i)] for i, at, _ in pieces]
        scores = [_dot(k_ref[here, _cols(i)], x, 1, 1) for (i, _, _), x in zip(pieces, qs)]
        dps = [_dot(v_ref[here, _cols(i)], x, 1, 1) for (i, _, _), x in zip(pieces, dos)]
        for n, (i, at, cut) in enumerate(pieces):
            p = jnp.exp2(scores[n] * e - lse_s[i : i + 1, at : at + wide])
            if cut:
                p = jnp.where(_mask(bk, wide, 0), p, 0.0)
            ds = (p * (dps[n] - delta_s[i : i + 1, at : at + wide])).astype(BF16)
            dv_s[i, here, :] += _dot(p.astype(BF16), dos[n])
            dk_s[i, here, :] += _dot(ds, qs[n])
            dq_s[i, :, at : at + wide] += _dot(k_ref[here, _cols(i)].T, ds)

    n = bq // bk
    lax.fori_loop(0, iq * n, lambda j, _: block(j, [(at, False) for at in range(0, bq, wide)]), None)
    for d in range(n):
        block(iq * n + d, [(at, at == d * bk) for at in range(d * bk, bq, wide)])
    for i in range(heads):
        dq_ref[:, _cols(i)] = _turn((dq_s[i] * scale).T.astype(BF16).astype(F32), cosq_ref[...], sinq_ref[...], True).astype(BF16)

    @pl.when(iq == pl.num_programs(1) - 1)
    def _():
        for i in range(heads):
            dk_ref[:, _cols(i)] = _turn((dk_s[i] * scale).astype(BF16).astype(F32), cos_ref[...], sin_ref[...], True).astype(BF16)
            dv_ref[:, _cols(i)] = dv_s[i].astype(BF16)


def attend_back(q, k, v, d_out, out, lse, cos, sin):
    t, width = q.shape
    heads, bq, bk = 2, min(1024, t), min(512, t)
    cols = heads * HEAD
    queries = ((bq, cols), lambda ih, iq: (iq, ih))
    keys = ((t, cols), lambda ih, iq: (0, ih))
    stats = ((1, heads, bq), lambda ih, iq: (ih, 0, iq))
    table_q = ((bq, HALF), lambda ih, iq: (iq, 0))
    table = ((t, HALF), lambda ih, iq: (0, 0), True)
    return _call(
        functools.partial(_attend_back, scale=HEAD**-0.5, bq=bq, bk=bk, heads=heads),
        "attend_back",
        (width // cols, t // bq),
        [queries, keys, keys, queries, queries, stats, table_q, table_q, table, table],
        [(*queries, (t, width), BF16), (*keys, (t, width), BF16), (*keys, (t, width), BF16)],
        [pltpu.VMEM((heads, HEAD, bq), F32), pltpu.VMEM((heads, t, HEAD), F32), pltpu.VMEM((heads, t, HEAD), F32),
         pltpu.VMEM((heads, bq), F32), pltpu.VMEM((heads, bq), F32)],
        5 * t * t * width,
        (q, k, v, d_out, out, lse.reshape(-1, heads, t), cos, sin, cos, sin),
    )


ROWS = 512
BLOCK = 512
PIECE = 512
TILE = 512


def _chunks(size, body):
    for at in range(0, size, ROWS):
        body(slice(at, at + ROWS))


def _scale_of(h):
    return lax.rsqrt(jnp.mean(h * h, axis=-1, keepdims=True) + 1e-6)


def _norm(h):
    return (h * _scale_of(h)).astype(BF16)


def _norm_back(by, h):
    r = _scale_of(h)
    return (by * r - h * (r * r * r * jnp.mean(by * h, axis=-1, keepdims=True))).astype(BF16)


def _qkv(h_ref, wq_ref, wk_ref, wv_ref, cos_ref, sin_ref, at_ref, q_ref, k_ref, v_ref):
    a = _norm(h_ref[...].astype(F32))
    at_ref[...] = a.T
    cos, sin = cos_ref[...], sin_ref[...]
    width = q_ref.shape[1]
    for at in range(0, width, PIECE):
        for w_ref, to_ref in ((wq_ref, q_ref), (wk_ref, k_ref)):
            t = _dot(a, w_ref[0, :, at : at + PIECE])
            for i in range(PIECE // HEAD):
                one = _turn(t[:, _cols(i)].astype(BF16).astype(F32), cos, sin)
                to_ref[:, at + i * HEAD : at + (i + 1) * HEAD] = one.astype(BF16)
        v_ref[:, at : at + PIECE] = _dot(a, wv_ref[0, :, at : at + PIECE]).astype(BF16)


def qkv(h, wq, wk, wv, cos, sin, number):
    t, d = h.shape
    width = wq.shape[2]
    rows = _row(BLOCK, d)
    wide = _row(BLOCK, width)
    w = _of_layer(number, d, width)
    table = _row(BLOCK, HALF)
    return _call(_qkv, "qkv", (t // BLOCK,), [rows, w, w, w, table, table],
                 [((d, BLOCK), lambda i: (0, i), (d, t), BF16)] + [(*wide, (t, width), BF16)] * 3, [], 6 * t * d * width, (h, wq, wk, wv, cos, sin))


def _out(h_ref, o_ref, w_ref, h2_ref, b_ref, bt_ref):
    h2 = (h_ref[...].astype(F32) + _dot(o_ref[...], w_ref[0]).astype(BF16).astype(F32)).astype(BF16)
    h2_ref[...] = h2
    b = _norm(h2.astype(F32))
    b_ref[...] = b
    bt_ref[...] = b.T


def out_and_norm(h, o, wo, number):
    t, d = h.shape
    width = o.shape[1]
    rows, wide = _row(BLOCK, d), _row(BLOCK, width)
    return _call(_out, "out", (t // BLOCK,), [rows, wide, _of_layer(number, width, d)],
                 [(*rows, (t, d), BF16)] * 2 + [((d, BLOCK), lambda i: (0, i), (d, t), BF16)], [], 2 * t * d * width, (h, o, wo))


def _mlp(b_ref, h_ref, wg_ref, wu_ref, wd_ref, g_ref, u_ref, to_ref, sum_s):
    f = pl.program_id(0)

    @pl.when(f == 0)
    def _():
        sum_s[...] = jnp.zeros_like(sum_s)

    def chunk(here):
        b = b_ref[here, :]
        g, u = _dot(b, wg_ref[0]), _dot(b, wu_ref[0])
        g_ref[here, :], u_ref[here, :] = g, u
        sum_s[here, :] += _dot((g * jax.nn.sigmoid(g) * u).astype(BF16), wd_ref[0])

    _chunks(b_ref.shape[0], chunk)

    @pl.when(f == pl.num_programs(0) - 1)
    def _():
        to_ref[...] = (h_ref[...].astype(F32) + sum_s[...].astype(BF16).astype(F32)).astype(BF16)


def _tiles(d, number):
    up = ((1, d, TILE), lambda i: (number, 0, i))
    down = ((1, TILE, d), lambda i: (number, i, 0))
    return up, down


def mlp(b, h, wg, wu, wd, number):
    t, d = b.shape
    ff = wg.shape[2]
    up, down = _tiles(d, number)
    whole = _still(t, d)
    hidden = _col(t, TILE)
    return _call(_mlp, "mlp", (ff // TILE,), [whole, whole, up, up, down],
                 [(*hidden, (t, ff), F32)] * 2 + [((t, d), lambda i: (0, 0), (t, d), BF16)], [pltpu.VMEM((t, d), F32)], 6 * t * d * ff,
                 (b, h, wg, wu, wd))


def _mlp_back(dh_ref, wd_ref, g_of, u_of, dg_ref, du_ref, dwd_ref, act_s):
    def chunk(here):
        g, u = g_of(here), u_of(here)
        by = _dot(dh_ref[here, :], wd_ref[0], 1, 1).astype(BF16).astype(F32)
        s = jax.nn.sigmoid(g)
        silu = g * s
        act_s[here, :] = (silu * u).astype(BF16)
        du_ref[here, :] = (by * silu).astype(BF16)
        dg_ref[here, :] = (by * u * (s + silu * (1 - s))).astype(BF16)

    _chunks(dh_ref.shape[0], chunk)
    dwd_ref[...] = _dot(act_s[...].T, dh_ref[...]).astype(BF16)


def _mlp_back_anew(b_ref, dh_ref, wg_ref, wu_ref, wd_ref, *rest):
    _mlp_back(dh_ref, wd_ref, lambda here: _dot(b_ref[here, :], wg_ref[0]), lambda here: _dot(b_ref[here, :], wu_ref[0]), *rest)


def _mlp_back_kept(g_ref, u_ref, dh_ref, wd_ref, *rest):
    _mlp_back(dh_ref, wd_ref, lambda here: g_ref[here, :], lambda here: u_ref[here, :], *rest)


def mlp_back(kept, dh, wg, wu, wd, number):
    t, d = dh.shape
    ff = wg.shape[2]
    up, down = _tiles(d, number)
    whole = _still(t, d)
    hidden = _col(t, TILE)
    if len(kept) == 2:
        kernel, ins, args, work = _mlp_back_kept, [hidden, hidden, whole, down], (*kept, dh, wd), 4
    else:
        kernel, ins, args, work = _mlp_back_anew, [whole, whole, up, up, down], (*kept, dh, wg, wu, wd), 8
    return _call(kernel, "mlp_back", (ff // TILE,), ins,
                 [(*hidden, (t, ff), BF16)] * 2 + [((TILE, d), lambda i: (i, 0), (ff, d), BF16)], [pltpu.VMEM((t, TILE), BF16)],
                 work * t * d * ff, args)


def _up_grad(dg_ref, du_ref, bt_ref, dw_ref):
    n, d = dw_ref.shape[0], bt_ref.shape[0]
    for i, ref in enumerate((dg_ref, du_ref)):
        dw_ref[:, i] = _dot(bt_ref[...], ref[...]).astype(BF16).reshape(n, d // n, TILE)


def up_grad(dg, du, bt, n):
    d, t = bt.shape
    ff = dg.shape[1]
    hidden = _col(t, TILE)
    return _call(_up_grad, "up_grad", (ff // TILE,), [hidden, hidden, _still(d, t)],
                 [((n, 2, d // n, TILE), lambda i: (0, 0, 0, i), (n, 2, d // n, ff), BF16)], [], 4 * t * d * ff, (dg, du, bt))[0]


def _up_back(dg_ref, du_ref, h_ref, dh_ref, wg_ref, wu_ref, wo_ref, dh2_ref, do_ref, sum_s):
    f = pl.program_id(0)

    @pl.when(f == 0)
    def _():
        sum_s[...] = jnp.zeros_like(sum_s)

    def chunk(here):
        sum_s[here, :] += _dot(dg_ref[here, :], wg_ref[0], 1, 1) + _dot(du_ref[here, :], wu_ref[0], 1, 1)

    _chunks(h_ref.shape[0], chunk)

    def last(here):
        back = _norm_back(sum_s[here, :].astype(BF16).astype(F32), h_ref[here, :].astype(F32))
        dh2 = (dh_ref[here, :].astype(F32) + back.astype(F32)).astype(BF16)
        dh2_ref[here, :] = dh2
        do_ref[here, :] = _dot(dh2, wo_ref[0], 1, 1).astype(BF16)

    @pl.when(f == pl.num_programs(0) - 1)
    def _():
        _chunks(h_ref.shape[0], last)


def up_back(dg, du, h, dh, wg, wu, wo, number):
    t, d = h.shape
    ff, width = wg.shape[2], wo.shape[1]
    up, _ = _tiles(d, number)
    whole = _still(t, d)
    hidden = _col(t, TILE)
    return _call(_up_back, "up_back", (ff // TILE,), [hidden, hidden, whole, whole, up, up, _of_layer(number, width, d)],
                 [((t, d), lambda i: (0, 0), (t, d), BF16), ((t, width), lambda i: (0, 0), (t, width), BF16)],
                 [pltpu.VMEM((t, d), F32)], 4 * t * d * ff, (dg, du, h, dh, wg, wu, wo))


def _qkv_back(at_ref, dq_ref, dk_ref, dv_ref, o_ref, dh2_ref, *rest, further):
    if further:
        h_ref, wq_ref, wk_ref, wv_ref, dw_ref, dh_ref, sum_s = rest
    else:
        dw_ref, sum_s = rest
    f = pl.program_id(0)
    n = dw_ref.shape[0]
    at, ot = at_ref[...], o_ref[...].T
    for i, (x, ref) in enumerate(((at, dq_ref), (at, dk_ref), (at, dv_ref), (ot, dh2_ref))):
        term = _dot(x, ref[...])
        sum_s[i] = jnp.where(f == 0, term, sum_s[i] + term)
    if further:
        by = _dot(dq_ref[...], wq_ref[0], 1, 1) + _dot(dk_ref[...], wk_ref[0], 1, 1) + _dot(dv_ref[...], wv_ref[0], 1, 1)
        back = _norm_back(by.astype(BF16).astype(F32), h_ref[...].astype(F32))
        dh_ref[...] = (dh2_ref[...].astype(F32) + back.astype(F32)).astype(BF16)

    @pl.when(f == pl.num_programs(0) - 1)
    def _():
        for i in range(4):
            dw_ref[:, i] = sum_s[i].astype(BF16).reshape(n, -1, dw_ref.shape[3])


def qkv_back(at, dq, dk, dv, o, dh2, h, wq, wk, wv, n, number):
    d, t = at.shape
    width = dq.shape[1]
    rows = _row(BLOCK, d)
    w = _of_layer(number, d, width)
    ins, outs, args = [_col(d, BLOCK)] + [rows] * 5, [((n, 4, d // n, width), lambda i: (0, 0, 0, 0), (n, 4, d // n, width), BF16)], (at, dq, dk, dv, o, dh2)
    further = number > 0
    if further:
        ins, outs, args = ins + [rows, w, w, w], outs + [(*rows, (t, d), BF16)], (*args, h, wq, wk, wv)
    return _call(functools.partial(_qkv_back, further=further), "qkv_back", (t // BLOCK,), ins, outs, [pltpu.VMEM((4, d, width), F32)],
                 (14 if further else 8) * t * d * width, args)


def _places(layout):
    me = lax.axis_index("dp")
    x, y, core = lax.div(me, 4), lax.rem(lax.div(me, 2), 2), lax.rem(me, 2)
    place = lambda x, y, core: layout(x, y, core)
    return core, place(x, y, core), place(1 - x, y, core), place(x, 1 - y, core), place(1 - x, 1 - y, core), place(x, y, 1 - core)


def _device(x, y, core):
    return x * 4 + y * 2 + core


def _chip(x, y, core):
    return x * 2 + y


def _meet(*peers):
    barrier = pltpu.get_barrier_semaphore()
    for peer in peers:
        pl.semaphore_signal(barrier, inc=1, device_id={"dp": peer}, device_id_type=pl.DeviceIdType.MESH)
    pl.semaphore_wait(barrier, len(peers))


def _scatter(x_ref, *refs, early):
    early_refs, (out_ref, squares_ref, core_s, to_x_s, to_y_s, from_x_s, from_y_s, on_y_s, on_x_s, last_y_s, last_x_s, send_sem, recv_sem) = (
        refs[:early], refs[early:])
    core, me, across_x, across_y, _, partner = _places(_device)
    _, chip, chip_x, chip_y, chip_d, _ = _places(_chip)
    _meet(across_x, across_y, partner)

    def send(i, src, dst, peer):
        copy = pltpu.make_async_remote_copy(src_ref=src, dst_ref=dst, send_sem=send_sem.at[i], recv_sem=recv_sem.at[i],
                                            device_id={"dp": peer}, device_id_type=pl.DeviceIdType.MESH)
        copy.start()
        return copy

    order = (chip_d, chip_x, chip_y, chip)
    swaps = [send(i, x_ref.at[to, 1 - core], core_s.at[to], partner) for i, to in enumerate(order)]
    first, second = slice(0, 2), slice(2, 4)

    def on_chip(to, half):
        return x_ref[to, core, half].astype(F32) + core_s[to, half].astype(F32)

    swaps[0].wait()
    to_x_s[1], to_y_s[1] = on_chip(chip_d, first).astype(BF16), on_chip(chip_d, second).astype(BF16)
    by_x = [send(4, to_x_s.at[1], from_x_s.at[1], across_x)]
    swaps[1].wait()
    to_x_s[0] = on_chip(chip_x, first).astype(BF16)
    by_y = [send(5, to_y_s.at[1], from_y_s.at[1], across_y)]
    swaps[2].wait()
    to_y_s[0] = on_chip(chip_y, second).astype(BF16)
    by_x.append(send(6, to_x_s.at[0], from_x_s.at[0], across_x))
    swaps[3].wait()
    by_y.append(send(7, to_y_s.at[0], from_y_s.at[0], across_y))
    squares = jnp.zeros((), F32)
    for ref in early_refs:
        squares += jnp.sum(jnp.square(ref[...].astype(F32)))
    by_x[0].wait()
    on_y_s[...] = (on_chip(chip_y, first) + from_x_s[1].astype(F32)).astype(BF16)
    by_y[0].wait()
    on_x_s[...] = (on_chip(chip_x, second) + from_y_s[1].astype(F32)).astype(BF16)
    then_y, then_x = send(8, on_y_s, last_y_s, across_y), send(9, on_x_s, last_x_s, across_x)
    for one, copy, half, came, last in ((by_x, then_y, first, from_x_s, last_y_s), (by_y, then_x, second, from_y_s, last_x_s)):
        one[1].wait()
        copy.wait()
        done = (on_chip(chip, half) + came[0].astype(F32) + last[...].astype(F32)).astype(BF16)
        out_ref[0, half] = done
        squares += jnp.sum(jnp.square(done.astype(F32)))
    squares_ref[...] = jnp.full(squares_ref.shape, squares)


def scatter(x, early):
    n, four, rows, cols = x.shape
    half = pltpu.VMEM((2, rows, cols), BF16)
    pair = pltpu.VMEM((2, 2, rows, cols), BF16)
    vmem = pl.BlockSpec(memory_space=pltpu.VMEM)
    return pl.pallas_call(
        functools.partial(_scatter, early=len(early)),
        name="scatter",
        in_specs=[vmem] * (1 + len(early)),
        out_specs=[vmem, vmem],
        out_shape=[jax.ShapeDtypeStruct((1, four, rows, cols), BF16), jax.ShapeDtypeStruct((8, 128), F32)],
        scratch_shapes=[pltpu.VMEM((4, four, rows, cols), BF16), pair, pair, pair, pair, half, half, half, half,
                        pltpu.SemaphoreType.DMA((10,)), pltpu.SemaphoreType.DMA((10,))],
        compiler_params=pltpu.CompilerParams(collective_id=1, has_side_effects=True, vmem_limit_bytes=VMEM),
        cost_estimate=pl.CostEstimate(flops=2**34, transcendentals=0, bytes_accessed=2 * x.size),
    )(x.reshape(4, 2, four, rows, cols), *early)


def _gather(*refs, count):
    x_refs, out_refs, (own_sem, send_sem, recv_sem) = refs[:count], refs[count : 2 * count], refs[2 * count :]
    _, me, across_x, across_y, across, partner = _places(_device)
    _meet(across_x, across_y, partner)
    owns = [pltpu.make_async_copy(x_ref, out_ref.at[me], own_sem.at[i]) for i, (x_ref, out_ref) in enumerate(zip(x_refs, out_refs))]
    for own in owns:
        own.start()
    sent = []

    def send(i, src, dst, peer):
        at = len(sent)
        copy = pltpu.make_async_remote_copy(src_ref=src, dst_ref=dst, send_sem=send_sem.at[at], recv_sem=recv_sem.at[at],
                                            device_id={"dp": peer}, device_id_type=pl.DeviceIdType.MESH)
        copy.start()
        sent.append(copy)
        return copy

    def pass_on(i, device, peer, half=None):
        block = out_refs[i].at[device] if half is None else out_refs[i].at[device, half]
        return send(i, block, block, peer)

    each = range(count)
    halves = [(slice(0, ref.shape[0] // 2), slice(ref.shape[0] // 2, ref.shape[0])) for ref in x_refs]
    to_x = [send(i, x_refs[i], out_refs[i].at[me], across_x) for i in each]
    to_y = [send(i, x_refs[i], out_refs[i].at[me], across_y) for i in each]
    to_core = [send(i, x_refs[i], out_refs[i].at[me], partner) for i in each]
    on_y, on_x = [], []
    for i in each:
        to_x[i].wait_recv()
        on_y.append(pass_on(i, across_x, across_y, halves[i][0]))
        to_core.append(pass_on(i, across_x, partner))
        to_y[i].wait_recv()
        on_x.append(pass_on(i, across_y, across_x, halves[i][1]))
        to_core.append(pass_on(i, across_y, partner))
    for i in each:
        on_y[i].wait_recv()
        to_core.append(pass_on(i, across, partner, halves[i][0]))
        on_x[i].wait_recv()
        to_core.append(pass_on(i, across, partner, halves[i][1]))
    for copy in to_core:
        copy.wait_recv()
    for copy in sent:
        copy.wait_send()
    for own in owns:
        own.wait()


def gather(*xs):
    anywhere = pl.BlockSpec(memory_space=pl.ANY)
    count = len(xs)
    sems = pltpu.SemaphoreType.DMA((9 * count,))
    return pl.pallas_call(
        functools.partial(_gather, count=count),
        name="gather",
        in_specs=[anywhere] * count,
        out_specs=[anywhere] * count,
        out_shape=[jax.ShapeDtypeStruct((8, *x.shape), x.dtype) for x in xs],
        scratch_shapes=[pltpu.SemaphoreType.DMA((count,)), sems, sems],
        compiler_params=pltpu.CompilerParams(collective_id=2, has_side_effects=True, vmem_limit_bytes=VMEM),
        cost_estimate=pl.CostEstimate(flops=2**34, transcendentals=0, bytes_accessed=2**25),
    )(*xs)


def _total(x_ref, sum_ref, got_s, send_sem, recv_sem, *, n):
    me = lax.axis_index("dp")
    peers = [lax.rem(me + k, n) for k in range(1, n)]
    barrier = pltpu.get_barrier_semaphore()
    for peer in peers:
        pl.semaphore_signal(barrier, inc=1, device_id={"dp": peer}, device_id_type=pl.DeviceIdType.MESH)
    pl.semaphore_wait(barrier, n - 1)
    copies = []
    for k, peer in enumerate(peers):
        copies.append(pltpu.make_async_remote_copy(src_ref=x_ref, dst_ref=got_s.at[k], send_sem=send_sem.at[k], recv_sem=recv_sem.at[k],
                                                   device_id={"dp": peer}, device_id_type=pl.DeviceIdType.MESH))
        copies[-1].start()
    for copy in copies:
        copy.wait()
    total = jnp.zeros(x_ref.shape, F32)
    for device in range(n):
        one = x_ref[...]
        for k in range(n - 1):
            one = jnp.where(lax.rem(me + n - k - 1, n) == device, got_s[k], one)
        total = total + one
    sum_ref[...] = total


def total(x, n):
    shape = (8, 128)
    return pl.pallas_call(
        functools.partial(_total, n=n),
        name="total",
        in_specs=[pl.BlockSpec(memory_space=pltpu.VMEM)],
        out_specs=pl.BlockSpec(memory_space=pltpu.VMEM),
        out_shape=jax.ShapeDtypeStruct(shape, F32),
        scratch_shapes=[pltpu.VMEM((n - 1, *shape), F32), pltpu.SemaphoreType.DMA((n - 1,)), pltpu.SemaphoreType.DMA((n - 1,))],
        compiler_params=pltpu.CompilerParams(collective_id=0, has_side_effects=True),
    )(jnp.full(shape, x))


def _adamw(me_ref, squares_ref, *refs, count, size):
    ws, ms, vs, refs = refs[:count], refs[count : 2 * count], refs[2 * count : 3 * count], refs[3 * count :]
    layers = ws[0].shape[0]
    grads, refs = refs[:layers], refs[layers:]
    sents, refs = (refs[:1], refs[1:]) if count > 1 else (refs[:layers], refs[layers:])
    new_ms, new_vs = refs[:count], refs[count:]
    factor = jnp.minimum(1.0, 0.5 * lax.rsqrt(squares_ref[0:1, 0:1] / size + 1e-30))
    for i in range(count):
        for layer in range(layers):
            g = (grads[layer][0, i] if count > 1 else grads[layer][...]).astype(F32) * factor
            m = 0.9 * ms[i][layer] + 0.1 * g
            v = 0.95 * vs[i][layer] + 0.05 * g * g
            w = ws[i][layer].astype(F32)
            new_ms[i][layer], new_vs[i][layer] = m, v
            to = sents[0].at[i, layer] if count > 1 else sents[layer]
            to[...] = (w - 0.02 * (m * lax.rsqrt(v + 1e-8) + 0.1 * w)).astype(BF16)


def adamw(me, squares, ws, ms, vs, grads, size, tile):
    count = len(ws)
    layers, rows, cols = ms[0].shape
    if count > 1:
        steps, block = cols // tile, (layers, rows, tile)
        mine = lambda i, me: (0, 0, i)
        theirs = lambda i, me: (0, me[0], i)
        grad = pl.BlockSpec((1, count, rows, tile), lambda i, me: (0, 0, 0, i))
        outs = [pl.BlockSpec((count, layers, rows, tile), lambda i, me: (0, 0, 0, i))]
        sent_shape = (count, *ms[0].shape)
    else:
        steps, block = rows // tile, (layers, tile, cols)
        mine = lambda i, me: (0, i, 0)
        theirs = lambda i, me: (0, me[0] * (rows // tile) + i, 0)
        grad = pl.BlockSpec((tile, cols), lambda i, me: (i, 0))
        outs = [grad] * layers
        sent_shape = (rows, cols)
    moment, weight = pl.BlockSpec(block, mine), pl.BlockSpec(block, theirs)
    shape = jax.ShapeDtypeStruct(ms[0].shape, F32)
    many = len(outs)
    got = pl.pallas_call(
        functools.partial(_adamw, count=count, size=size),
        name="adamw",
        grid_spec=pltpu.PrefetchScalarGridSpec(
            num_scalar_prefetch=1,
            grid=(steps,),
            in_specs=[pl.BlockSpec((8, 128), lambda i, me: (0, 0))] + [weight] * count + [moment] * (2 * count) + [grad] * layers,
            out_specs=outs + [moment] * (2 * count),
        ),
        out_shape=[jax.ShapeDtypeStruct(sent_shape, BF16)] * many + [shape] * (2 * count),
        compiler_params=pltpu.CompilerParams(dimension_semantics=("arbitrary",), vmem_limit_bytes=VMEM),
        cost_estimate=pl.CostEstimate(flops=20 * count * ms[0].size, transcendentals=0, bytes_accessed=22 * count * ms[0].size),
    )(me, squares, *ws, *ms, *vs, *grads)
    return got[:many], got[many : many + count], got[many + count :]


def _unpack(got_ref, *w_refs):
    for i, ref in enumerate(w_refs):
        ref[...] = got_ref[0, i]


def unpack(got):
    n, count, layers, rows, cols = got.shape
    return _call(_unpack, "unpack", (n,), [((1, count, layers, rows, cols), lambda i: (i, 0, 0, 0, 0))],
                 [((layers, rows, cols), lambda i: (0, i, 0), (layers, n * rows, cols), BF16)] * count, [], got.size, (got,))


def _place_layer(got_ref, *refs):
    refs[-1][...] = got_ref[...][None]


def place_layer(got, layer, layers, others=None):
    rows, cols = got.size // got.shape[-1], got.shape[-1]
    ins, args = [pl.BlockSpec(*_row(ROWS, cols))], [got.reshape(rows, cols)]
    if others is not None:
        ins, args = ins + [pl.BlockSpec(memory_space=pl.ANY)], args + [others]
    return pl.pallas_call(
        _place_layer,
        name="place_layer",
        grid=(rows // ROWS,),
        in_specs=ins,
        out_specs=pl.BlockSpec((1, ROWS, cols), lambda i: (layer, i, 0)),
        out_shape=jax.ShapeDtypeStruct((layers, rows, cols), got.dtype),
        input_output_aliases={} if others is None else {1: 0},
        compiler_params=pltpu.CompilerParams(dimension_semantics=("arbitrary",), vmem_limit_bytes=VMEM),
        cost_estimate=pl.CostEstimate(flops=got.size, transcendentals=0, bytes_accessed=4 * got.size),
    )(*args)


def solution(mesh):
    n = mesh.shape["dp"]

    def scattered(x):
        return lax.psum_scatter(x, "dp", scatter_dimension=0, tiled=True)

    def step(x, dy, *arrays):
        weights, m, v = (arrays[i : i + 7] for i in (0, 7, 14))
        wq, wk, wv, wo, wg, wu, wd = weights
        layers = wq.shape[0]
        t = x.shape[1]
        angle = np.arange(t, dtype=np.float32)[:, None] * np.float32(THETA) ** (-np.arange(HALF, dtype=np.float32) / np.float32(HALF))
        cos, sin = (jnp.asarray(f(angle.astype(np.float64)).astype(np.float32)) for f in (np.cos, np.sin))
        h, kept = x[0], []
        for number in range(layers):
            at, q, k, v_ = qkv(h, wq, wk, wv, cos, sin, number)
            o, lse = attend(q, k, v_)
            h2, b, bt = out_and_norm(h, o, wo, number)
            last = number == layers - 1
            hidden = (b,)
            if not last:
                *hidden, after = mlp(b, h2, wg, wu, wd, number)
            kept.append((h, at, q, k, v_, o, lse, h2, bt, hidden))
            h = None if last else after
        by_h, ends, got = dy[0], [], []

        def waited(x):
            done, x = lax.optimization_barrier((ends.pop(0), x))
            got.append(done)
            return x

        for number in reversed(range(layers)):
            h, at, q, k, v_, o, lse, h2, bt, hidden = kept[number]
            if ends:
                by_h = waited(by_h)
            dg, du, by_down = mlp_back(hidden, by_h, wg, wu, wd, number)
            ends.append(scattered(by_down))
            by_up = up_grad(dg, du, bt, n)
            if len(ends) > 1:
                dg = waited(dg)
            ends.append(scattered(by_up))
            by_h2, by_o = up_back(dg, du, h2, by_h, wg, wu, wo, number)
            by_o = waited(by_o)
            dq, dk, dv = attend_back(q, k, v_, by_o, o, lse, cos, sin)
            by_attention, *by_h = qkv_back(at, dq, dk, dv, o, by_h2, h, wq, wk, wv, n, number)
            by_h = by_h[0] if by_h else None
            if number > 0:
                ends.append(scattered(by_attention))
        by_attention, squares = scatter(by_attention, got)
        squares = waited(squares)
        squares = squares[0, 0] + jnp.sum(jnp.square(got[-1].astype(F32)))
        got.append(by_attention)
        squares = total(squares, n)
        me = lax.axis_index("dp").astype(jnp.int32)[None]
        size = n * sum(one.size for one in m)
        new_m, new_v, sent = [None] * 7, [None] * 7, []
        groups = (((4, 5), 1, 512), ((6,), 0, 128), ((0, 1, 2, 3), 2, 512))
        for group, place, tile in groups:
            grads = [got[3 * (layers - 1 - number) + place] for number in range(layers)]
            one, some_m, some_v = adamw(me, squares, *([a[i] for i in group] for a in (weights, m, v)), grads, size, tile)
            one, squares = lax.optimization_barrier((one, squares))
            sent.append(one)
            for i, m_, v_ in zip(group, some_m, some_v):
                new_m[i], new_v[i] = m_, v_
        (up,), (down, last_down), (attention,) = sent
        up, last_down = lax.all_gather(up, "dp"), lax.all_gather(last_down, "dp", tiled=True)
        attention, down = gather(attention, down)
        attention, down = unpack(attention), place_layer(down, 0, layers)
        up, attention, down = lax.optimization_barrier((up, attention, down))
        up = unpack(up)
        last_down, up = lax.optimization_barrier((last_down, up))
        whole = (*attention, *up, place_layer(last_down, layers - 1, layers, down))
        return (*whole, *new_m, *new_v)

    states, all_of, cut = P(("rep", "dp"), None, None), P(None, None, None), P(None, "dp", None)
    return jax.shard_map(
        step,
        mesh=mesh,
        in_specs=(states, states) + (all_of,) * 7 + (cut,) * 14,
        out_specs=(P("rep", None, None),) * 7 + (P("rep", "dp", None),) * 14,
        check_vma=False,
    )
```
